32 devices in a mesh: dp: 1 (over z), sw: 4 (over y), sh: 8 (over x, core).
Axes of the slice: x: 4, y: 4, z: 1, core: 2. Of those that a mesh axis runs over, the one named last changes fastest.
The devices are a block of a 4x4x8 slice.
Arguments:
- act_in: bfloat16 [24, 192, 48, 80], P('dp', 'sh', 'sw')
- drop_mask: float32 [24, 2], P('dp')
- grad_out: bfloat16 [24, 192, 48, 80], P('dp', 'sh', 'sw')
- conv_w: bfloat16 [2, 7, 7, 80], replicated
- conv_b: float32 [2, 80], replicated
- norm_g: float32 [2, 80], replicated
- norm_b: float32 [2, 80], replicated
- fc1_w: bfloat16 [2, 80, 320], replicated
- fc1_b: float32 [2, 320], replicated
- grn_gamma: float32 [2, 320], replicated
- grn_beta: float32 [2, 320], replicated
- fc2_w: bfloat16 [2, 320, 80], replicated
- fc2_b: float32 [2, 80], replicated
Outputs:
- output 1: bfloat16 [24, 192, 48, 80], P('dp', 'sh', 'sw')
- output 2: bfloat16 [24, 192, 48, 80], P('dp', 'sh', 'sw')
- output 3: float32 [2, 7, 7, 80], P('dp')
- output 4: float32 [2, 80], P('dp')
- output 5: float32 [2, 80], P('dp')
- output 6: float32 [2, 80], P('dp')
- output 7: float32 [2, 80, 320], P('dp')
- output 8: float32 [2, 320], P('dp')
- output 9: float32 [2, 320], P('dp')
- output 10: float32 [2, 320], P('dp')
- output 11: float32 [2, 320, 80], P('dp')
- output 12: float32 [2, 80], P('dp')
All inputs are finite; a program needn't handle non-finite values.
Results may differ from the reference program's by a relative error of at most 0.0133864.
Values are sent between devices in bfloat16 or wider.
A program may use at most 768 MiB of HBM per device.

```python
import jax
import jax.numpy as jnp
from jax import lax

BATCH = 24
GRID_H = 8
GRID_W = 4
TILE_H = 24
TILE_W = 12
CHANNELS = 80

HEIGHT = TILE_H * GRID_H
WIDTH = TILE_W * GRID_W
HIDDEN = 4 * CHANNELS
N_DROP = max(1, BATCH // 4)
KEEP_SCALE = 4.0 / 3.0
EPSILON = 1e-6


def setup_inputs(seed: int = 0, part: int = 0) -> dict:
    root_key = jax.random.key(seed)
    shared = jax.random.split(root_key, 10)
    part_keys = jax.random.split(jax.random.fold_in(root_key, part), 6)
    img_shape = (BATCH, HEIGHT, WIDTH, CHANNELS)
    tile_shape = (BATCH, GRID_H, GRID_W, CHANNELS)

    def spread(tile_vals):
        return jnp.repeat(jnp.repeat(tile_vals, TILE_H, axis=1), TILE_W, axis=2)

    def normal(index, shape):
        return jax.random.normal(shared[index], shape, jnp.float32)

    images = jax.random.normal(part_keys[0], img_shape, jnp.float32) + 1.5 * spread(jax.random.normal(part_keys[1], tile_shape, jnp.float32))
    cotangent = (jax.random.normal(part_keys[2], img_shape, jnp.float32)
                 + 0.8 * spread(jax.random.normal(part_keys[3], tile_shape, jnp.float32))
                 + 0.6 * jax.random.normal(part_keys[4], (BATCH, 1, 1, CHANNELS), jnp.float32))
    mask_keys = jax.random.split(part_keys[5], 2)
    drop_rank = jnp.stack([jax.random.permutation(mask_keys[0], BATCH), jax.random.permutation(mask_keys[1], BATCH)], axis=1)
    drop_mask = jnp.where(drop_rank < N_DROP, 0.0, KEEP_SCALE).astype(jnp.float32)
    return dict(
        act_in=images.astype(jnp.bfloat16),
        drop_mask=drop_mask,
        grad_out=cotangent.astype(jnp.bfloat16),
        conv_w=(normal(0, (2, 7, 7, CHANNELS)) / 7.0).astype(jnp.bfloat16),
        conv_b=0.5 * normal(1, (2, CHANNELS)),
        norm_g=1.0 + 0.3 * normal(2, (2, CHANNELS)),
        norm_b=0.3 * normal(3, (2, CHANNELS)),
        fc1_w=(normal(4, (2, CHANNELS, HIDDEN)) * CHANNELS ** -0.5).astype(jnp.bfloat16),
        fc1_b=0.5 * normal(5, (2, HIDDEN)),
        grn_gamma=normal(6, (2, HIDDEN)),
        grn_beta=0.5 * normal(7, (2, HIDDEN)),
        fc2_w=(normal(8, (2, HIDDEN, CHANNELS)) * HIDDEN ** -0.5).astype(jnp.bfloat16),
        fc2_b=0.5 * normal(9, (2, CHANNELS)),
    )


def convnext_block(x_img, mask_val, weights):
    conv_w, conv_b, norm_g, norm_b, fc1_w, fc1_b, grn_gamma, grn_beta, fc2_w, fc2_b = weights
    x_float = x_img.astype(jnp.float32)
    conv_out = lax.conv_general_dilated(x_float[None], conv_w[:, :, None, :], (1, 1), ((3, 3), (3, 3)),
                                        dimension_numbers=('NHWC', 'HWIO', 'NHWC'),
                                        feature_group_count=CHANNELS)[0]
    conv_out = (conv_out + conv_b).astype(jnp.bfloat16).astype(jnp.float32)
    centered = conv_out - jnp.mean(conv_out, axis=-1, keepdims=True)
    normed = centered * lax.rsqrt(jnp.mean(centered * centered, axis=-1, keepdims=True) + EPSILON)
    n_act = (normed * norm_g + norm_b).astype(jnp.bfloat16).astype(jnp.float32)
    hidden = (jnp.einsum('hwc,ck->hwk', n_act, fc1_w) + fc1_b).astype(jnp.bfloat16).astype(jnp.float32)
    g_act = jax.nn.gelu(hidden, approximate=False)
    g_norm = jnp.sqrt(jnp.sum(g_act * g_act, axis=(0, 1)))
    grn_scale = g_norm / (jnp.mean(g_norm) + EPSILON)
    grn_out = (grn_gamma * (g_act * grn_scale) + grn_beta + g_act).astype(jnp.bfloat16).astype(jnp.float32)
    proj_out = jnp.einsum('hwk,kc->hwc', grn_out, fc2_w) + fc2_b
    return (x_float + mask_val * proj_out).astype(jnp.bfloat16)


def two_blocks(x_img, mask_row, weights):
    first_w = tuple(weight[0] for weight in weights)
    second_w = tuple(weight[1] for weight in weights)
    return convnext_block(convnext_block(x_img, mask_row[0], first_w), mask_row[1], second_w)


def reference(act_in, drop_mask, grad_out, conv_w, conv_b, norm_g, norm_b, fc1_w, fc1_b, grn_gamma, grn_beta, fc2_w, fc2_b):
    params = tuple(weight.astype(jnp.float32) for weight in (conv_w, conv_b, norm_g, norm_b, fc1_w, fc1_b, grn_gamma, grn_beta, fc2_w, fc2_b))

    def one_image(image_item):
        x_img, mask_row, d_img = image_item

        def forward(x_in, weights):
            return two_blocks(x_in, mask_row, weights)

        out_img, pullback = jax.vjp(forward, x_img, params)
        d_x, d_weights = pullback(d_img)
        return out_img, d_x, d_weights

    act_out, grad_in, weight_grads = lax.map(one_image, (act_in, drop_mask, grad_out))
    return (act_out, grad_in) + tuple(jnp.sum(per_image, axis=0) for per_image in weight_grads)
```

```python
import functools

import jax
import jax.numpy as jnp
import numpy as np
from jax import lax
from jax.experimental import pallas as pl
from jax.experimental.pallas import tpu as pltpu
from jax.sharding import PartitionSpec as P

EPSILON = 1e-6
RADIUS = 3
TAPS = 2 * RADIUS + 1
MESH = pl.DeviceIdType.MESH
F32 = jnp.float32
BF16 = jnp.bfloat16
KEEP = 4.0 / 3.0
VMEM_LIMIT = 60 * 1024 * 1024
FULL = pl.BlockSpec(memory_space=pltpu.VMEM)


def round_up(value, unit):
    return (value + unit - 1) // unit * unit


class Dims:
    def __init__(self, act_shape, hidden):
        self.b, self.h, self.w, self.c = act_shape
        self.hid = hidden
        self.nw = self.w // RADIUS
        self.cp = round_up(RADIUS * self.c, 128)
        self.hp = round_up(RADIUS * hidden, 128)
        self.rw = self.nw * self.b
        self.rows = self.h * self.rw


def dot(lhs, rhs):
    return jnp.dot(lhs, rhs, preferred_element_type=F32)


def dot_t(lhs, rhs):
    return lax.dot_general(lhs, rhs, (((0,), (0,)), ((), ())), preferred_element_type=F32)


def dot_split(values, rhs):
    hi = values.astype(BF16)
    rest = values - hi.astype(F32)
    mid = rest.astype(BF16)
    low = (rest - mid.astype(F32)).astype(BF16)
    return dot(hi, rhs) + dot(mid, rhs) + dot(low, rhs)


def build_wide(dm, src_ref, wide):
    in_rows = (dm.nw + 2) * dm.b

    def body(row, carry):
        block = src_ref[pl.ds(pl.multiple_of(row * in_rows, 16), in_rows), :]
        for g in range(3):
            wide[pl.ds(pl.multiple_of(row * dm.rw, 16), dm.rw), g * dm.cp:(g + 1) * dm.cp] = block[g * dm.b:g * dm.b + dm.rw]
        return carry

    lax.fori_loop(0, dm.h + 2 * RADIUS, body, 0)


def build_toeplitz(dm, taps_ref, rel_ref, toep):
    def body(i, carry):
        for g in range(3):
            acc = jnp.zeros((dm.cp, dm.cp), F32)
            for dj in range(-2, 3):
                j = 3 * g + dj
                if 0 <= j < TAPS:
                    acc = jnp.where(rel_ref[...] == dj, taps_ref[pl.ds(i * 8 + j, 1), :], acc)
            toep[pl.ds(pl.multiple_of((i * 3 + g) * dm.cp, 16), dm.cp), :] = acc.astype(BF16)
        return carry

    lax.fori_loop(0, TAPS, body, 0)


def conv_tile(dm, wide, toep, first_row, th):
    m = th * dm.rw
    acc = None
    for i in range(TAPS):
        rows = pl.ds(pl.multiple_of((first_row + i) * dm.rw, 16), m)
        part = dot(wide[rows, :], toep[i * 3 * dm.cp:(i + 1) * 3 * dm.cp, :])
        acc = part if acc is None else acc + part
    return acc


def lane_loop(dm, th, body):
    def outer(r, carry):
        def inner(lane, c2):
            rows = pl.ds(pl.multiple_of(r * dm.rw, 16), dm.rw)
            body(rows, pl.ds(pl.multiple_of(lane * 128, 128), 128))
            return c2
        return lax.fori_loop(0, dm.hp // 128, inner, carry)
    lax.fori_loop(0, th, outer, 0)


def per_image(dm, values):
    return values.reshape(dm.nw, dm.b, values.shape[-1])


def phi_of(hv):
    return 0.5 + 0.5 * lax.erf(hv * np.float32(0.7071067811865476))


def forward_kernel(dm, th, second, *refs):
    (xp, taps, rel, conv_b, norm_g, norm_b, ones, w1, b1), refs = refs[:9], refs[9:]
    if second:
        (dout, w2t, mask), refs = refs[:3], refs[3:]
    (normed_o, inv_o, h_o, phi_o, ss_o), refs = refs[:5], refs[5:]
    if second:
        (dr_o, cross_o, sdr_o), refs = refs[:3], refs[3:]
    wide, toep = refs[:2]
    if second:
        raw = refs[2]
    step = pl.program_id(0)

    @pl.when(step == 0)
    def _():
        build_wide(dm, xp, wide)
        build_toeplitz(dm, taps, rel, toep)
        ss_o[...] = jnp.zeros_like(ss_o)
        if second:
            cross_o[...] = jnp.zeros_like(cross_o)
            sdr_o[...] = jnp.zeros_like(sdr_o)

    d = (conv_tile(dm, wide, toep, step * th, th) + conv_b[...]).astype(BF16)
    mean = dot(d, ones[...]) * np.float32(1.0 / dm.c)
    centered = d.astype(F32) - mean
    var = dot_split(centered * centered, ones[...]) * np.float32(1.0 / dm.c)
    inv = lax.rsqrt(var + EPSILON)
    normed = centered * inv
    normed_o[...] = normed
    inv_o[...] = inv
    n = (normed * norm_g[...] + norm_b[...]).astype(BF16)
    h_o[...] = (dot(n, w1[...]) + b1[...]).astype(BF16)
    if second:
        raw[...] = dot(dout[...], w2t[...])

    def body(rows, lanes):
        hv = h_o[rows, lanes].astype(F32)
        phi = phi_of(hv)
        phi_o[rows, lanes] = phi
        g = hv * phi
        ss_o[:, lanes] += jnp.sum(per_image(dm, g * g), axis=0)
        if second:
            dr = (per_image(dm, raw[rows, lanes]) * mask[:, :128][None]).astype(BF16)
            dr_o[rows, lanes] = dr.reshape(dm.rw, 128)
            dr32 = dr.astype(F32)
            cross_o[:, lanes] += jnp.sum(dr32 * per_image(dm, g), axis=0)
            sdr_o[:, lanes] += jnp.sum(dr32, axis=0)

    lane_loop(dm, th, body)


def response_kernel(dm, th, h_i, phi_i, coef, beta, w2, b2, x_i, mask, y_o, resp):
    def body(rows, lanes):
        g = h_i[rows, lanes].astype(F32) * phi_i[rows, lanes]
        r = per_image(dm, g) * coef[:, lanes][None] + beta[:, lanes][None]
        resp[rows, lanes] = r.reshape(dm.rw, 128).astype(BF16)

    lane_loop(dm, th, body)
    o = (dot(resp[...], w2[...]) + b2[...]).reshape(-1, dm.b, dm.cp)
    y_o[...] = (x_i[...].astype(F32) + (o * mask[...][None]).reshape(-1, dm.cp)).astype(BF16)


def backward_kernel(dm, th, second, *refs):
    (h_i, phi_i, dr_i, coef, dsq, beta, dout, mask, normed_i, inv_i, norm_g, norm_b, ones, gmat, w1t), refs = refs[:15], refs[15:]
    if second:
        (w2, b2, x_i), refs = refs[:3], refs[3:]
    (dconv_o, gfc1_o, gfc2_o, sdh_o, sums_o), refs = refs[:5], refs[5:]
    if second:
        y_o, refs = refs[0], refs[1:]
    resp, dh = refs
    step = pl.program_id(0)

    @pl.when(step == 0)
    def _():
        for ref in (gfc1_o, gfc2_o, sdh_o, sums_o):
            ref[...] = jnp.zeros_like(ref)

    def body(rows, lanes):
        hv = h_i[rows, lanes].astype(F32)
        phi = phi_i[rows, lanes]
        g = per_image(dm, hv * phi)
        a = coef[:, lanes][None]
        resp[rows, lanes] = (g * a + beta[:, lanes][None]).reshape(dm.rw, 128).astype(BF16)
        slope = phi + hv * (np.float32(0.3989422804014327) * jnp.exp(-0.5 * hv * hv))
        dg = per_image(dm, dr_i[rows, lanes].astype(F32)) * a + g * dsq[:, lanes][None]
        dhv = (dg.reshape(dm.rw, 128) * slope).astype(BF16)
        dh[rows, lanes] = dhv
        sdh_o[:, lanes] += jnp.sum(per_image(dm, dhv.astype(F32)), axis=0)

    lane_loop(dm, th, body)
    keep = (mask[...] != 0.0)[None]
    dsel32 = jnp.where(keep, dout[...].astype(F32).reshape(-1, dm.b, dm.cp), 0.0)
    sums_o[3] += jnp.sum(dsel32, axis=0)
    dsel = dsel32.reshape(-1, dm.cp).astype(BF16)
    gfc2_o[...] += dot_t(dsel, resp[...])
    if second:
        o = (dot(resp[...], w2[...]) + b2[...]).reshape(-1, dm.b, dm.cp)
        y_o[...] = (x_i[...].astype(F32) + (o * mask[...][None]).reshape(-1, dm.cp)).astype(BF16)
    normed = normed_i[...]
    n = (normed * norm_g[...] + norm_b[...]).astype(BF16)
    gfc1_o[...] += dot_t(n, dh[...])
    dn16 = dot(dh[...], w1t[...]).astype(BF16)
    dn = dn16.astype(F32)
    scale = np.float32(1.0 / dm.c)
    mean1 = (dot(dn16, gmat[0]) + dot(dn16, gmat[1]) + dot(dn16, gmat[2])) * scale
    dnormed = dn * norm_g[...]
    mean2 = dot_split(dnormed * normed, ones[...]) * scale
    dconv = (inv_i[...] * (dnormed - mean1 - normed * mean2)).astype(BF16)
    dconv_o[...] = dconv

    def fold(values):
        return jnp.sum(values.reshape(-1, dm.b, dm.cp), axis=0)

    sums_o[0] += fold(dconv.astype(F32))
    sums_o[1] += fold(dn * normed)
    sums_o[2] += fold(dn)


def input_grad_kernel(dm, th, last, *refs):
    (dp, taps, rel, dout), refs = refs[:4], refs[4:]
    if not last:
        (w2t, mask, h_i, phi_i), refs = refs[:4], refs[4:]
    din_o, refs = refs[0], refs[1:]
    if not last:
        (dr_o, cross_o, sdr_o), refs = refs[:3], refs[3:]
    wide, toep = refs[:2]
    step = pl.program_id(0)

    @pl.when(step == 0)
    def _():
        build_wide(dm, dp, wide)
        build_toeplitz(dm, taps, rel, toep)
        if not last:
            cross_o[...] = jnp.zeros_like(cross_o)
            sdr_o[...] = jnp.zeros_like(sdr_o)

    din = (dout[...].astype(F32) + conv_tile(dm, wide, toep, step * th, th)).astype(BF16)
    din_o[...] = din
    if not last:
        raw = refs[2]
        raw[...] = dot(din, w2t[...])

        def body(rows, lanes):
            g = h_i[rows, lanes].astype(F32) * phi_i[rows, lanes]
            dr = (per_image(dm, raw[rows, lanes]) * mask[:, :128][None]).astype(BF16)
            dr_o[rows, lanes] = dr.reshape(dm.rw, 128)
            dr32 = dr.astype(F32)
            cross_o[:, lanes] += jnp.sum(dr32 * per_image(dm, g), axis=0)
            sdr_o[:, lanes] += jnp.sum(dr32, axis=0)

        lane_loop(dm, th, body)


def wgrad_kernel(dm, xp, dconv, rel, out, wide, dcol):
    build_wide(dm, xp, wide)
    dcol[...] = dconv[...].T
    keep = rel[...] > -50

    def body(i, carry):
        rows = pl.ds(pl.multiple_of(i * dm.rw, 16), dm.rows)
        res = dot(dcol[...], wide[rows, :])
        for g in range(3):
            part = jnp.where(keep, res[:, g * dm.cp:(g + 1) * dm.cp], 0.0)
            for q in range(3):
                out[i, pl.ds(q, 1), g * dm.cp:(g + 1) * dm.cp] = jnp.sum(part[q * dm.c:(q + 1) * dm.c], axis=0, keepdims=True)
        return carry

    lax.fori_loop(0, TAPS, body, 0)


def position(grid):
    sh = lax.axis_index('sh')
    sw = lax.axis_index('sw')
    return sh // 2, sh % 2, sw


def peers_of(grid):
    chip, core, sw = position(grid)
    n_chip, n_sw = grid[0] // 2, grid[1]
    pair = {'sh': chip * 2 + 1 - core}
    row = [{'sh': lax.rem(chip + k, n_chip) * 2 + core} for k in range(1, n_chip)]
    col = [{'sw': lax.rem(sw + k, n_sw)} for k in range(1, n_sw)]
    return pair, row, col


def greet(pair, row, col):
    barrier = pltpu.get_barrier_semaphore()
    for device in [pair] + row + col:
        pl.semaphore_signal(barrier, inc=1, device_id=device, device_id_type=MESH)
    pl.semaphore_wait(barrier, 1 + len(row) + len(col))


def exchange(slots, mine, devices, send_sem, recv_sem):
    copies = []
    for k, device in enumerate(devices):
        copy = pltpu.make_async_remote_copy(src_ref=slots.at[mine], dst_ref=slots.at[mine], send_sem=send_sem.at[k],
                                            recv_sem=recv_sem.at[k], device_id=device, device_id_type=MESH)
        copy.start()
        copies.append(copy)
    for copy in copies:
        copy.wait()


def sum_slots(slots):
    total = slots[0]
    for k in range(1, slots.shape[0]):
        total = total + slots[k]
    return total


def grn_kernel(dm, grid, n_fwd, n_cross, *refs):
    sums, refs = refs[:n_fwd + n_cross], refs[n_fwd + n_cross:]
    if n_fwd == 0:
        norm_i, refs = refs[0], refs[1:]
    gamma, refs = refs[0], refs[1:]
    n_out = 2 * n_fwd + 2 * n_cross
    outs, refs = refs[:n_out], refs[n_out:]
    slots1, slots2, slots3, send1, recv1, send2, recv2, send3, recv3 = refs
    chip, core, sw = position(grid)
    pair, row, col = peers_of(grid)
    greet(pair, row, col)

    def fold(ref):
        return ref[:, :dm.hid] + ref[:, dm.hid:2 * dm.hid] + ref[:, 2 * dm.hid:3 * dm.hid]

    slots1[core] = jnp.stack([fold(ref) for ref in sums])
    exchange(slots1, core, [pair], send1, recv1)
    slots2[chip] = sum_slots(slots1)
    exchange(slots2, chip, row, send2, recv2)
    slots3[sw] = sum_slots(slots2)
    exchange(slots3, sw, col, send3, recv3)
    total = sum_slots(slots3)

    outs = list(outs)
    if n_fwd:
        norm = jnp.sqrt(total[0])
        outs.pop(0)[...] = norm
    else:
        norm = norm_i[...]
    mean = jnp.mean(norm, axis=-1, keepdims=True) + EPSILON
    scale = norm / mean

    def spread(ref, values):
        ref[...] = jnp.zeros_like(ref)
        for q in range(3):
            ref[:, q * dm.hid:(q + 1) * dm.hid] = values

    if n_fwd:
        spread(outs.pop(0), gamma[...] * scale + 1.0)
    if n_cross:
        cross = total[n_fwd]
        d_scale = gamma[...] * cross
        d_norm = d_scale / mean - jnp.sum(d_scale * norm, axis=-1, keepdims=True) / (mean * mean * dm.hid)
        spread(outs.pop(0), d_norm / norm)
        outs.pop(0)[...] = jnp.sum(cross * scale, axis=0, keepdims=True)


def grn_reduce(dm, grid, fwd, cross, norm, gamma, cid):
    n_fwd, n_cross = len(fwd), len(cross)
    count = n_fwd + n_cross
    wide = jax.ShapeDtypeStruct((dm.b, dm.hp), F32)
    outs = []
    if n_fwd:
        outs += [jax.ShapeDtypeStruct((dm.b, dm.hid), F32), wide]
    if n_cross:
        outs += [wide, jax.ShapeDtypeStruct((1, dm.hid), F32)]
    args = list(fwd) + list(cross) + ([] if n_fwd else [norm]) + [gamma]
    block = (count, dm.b, dm.hid)
    n_chip, n_sw = grid[0] // 2, grid[1]
    dma = pltpu.SemaphoreType.DMA
    return pl.pallas_call(
        functools.partial(grn_kernel, dm, grid, n_fwd, n_cross),
        out_shape=outs, in_specs=[FULL] * len(args), out_specs=[FULL] * len(outs),
        scratch_shapes=[pltpu.VMEM((2,) + block, F32), pltpu.VMEM((n_chip,) + block, F32), pltpu.VMEM((n_sw,) + block, F32),
                        dma((1,)), dma((1,)), dma((n_chip - 1,)), dma((n_chip - 1,)), dma((n_sw - 1,)), dma((n_sw - 1,))],
        compiler_params=pltpu.CompilerParams(collective_id=cid, has_side_effects=True),
        name=f'grn_reduce_{cid}',
    )(*args)


def sum_kernel(grid, x, out, half, got1, part, got2, slots3, *sems):
    send1, recv1, send2, recv2, send3, recv3, send4, recv4, send5, recv5 = sems
    chip, core, sw = position(grid)
    n_chip = grid[0] // 2
    pair, row, col = peers_of(grid)
    greet(pair, row, col)
    c1 = pltpu.make_async_remote_copy(src_ref=x.at[1 - core], dst_ref=got1, send_sem=send1.at[0], recv_sem=recv1.at[0],
                                      device_id=pair, device_id_type=MESH)
    c1.start()
    c1.wait()
    half[...] = x[core] + got1[...]
    copies = []
    for k, device in enumerate(row):
        target = lax.rem(chip + k + 1, n_chip)
        copy = pltpu.make_async_remote_copy(src_ref=half.at[target], dst_ref=got2.at[chip], send_sem=send2.at[k],
                                            recv_sem=recv2.at[k], device_id=device, device_id_type=MESH)
        copy.start()
        copies.append(copy)
    got2[chip] = half[chip]
    for copy in copies:
        copy.wait()
    slots3[sw] = sum_slots(got2)
    exchange(slots3, sw, col, send3, recv3)
    part[chip] = sum_slots(slots3)
    exchange(part, chip, row, send4, recv4)
    out[core] = part[...]
    c5 = pltpu.make_async_remote_copy(src_ref=part, dst_ref=out.at[core], send_sem=send5.at[0], recv_sem=recv5.at[0],
                                      device_id=pair, device_id_type=MESH)
    c5.start()
    c5.wait()


def sum_all(grid, flat, cid):
    n_chip, n_sw = grid[0] // 2, grid[1]
    size = flat.shape[0]
    lines = round_up(-(-size // (2 * n_chip * 128)), 8)
    x = jnp.pad(flat, (0, 2 * n_chip * lines * 128 - size)).reshape(2, n_chip, lines, 128)
    dma = pltpu.SemaphoreType.DMA
    block = (lines, 128)
    out = pl.pallas_call(
        functools.partial(sum_kernel, grid),
        out_shape=jax.ShapeDtypeStruct(x.shape, F32), in_specs=[FULL], out_specs=FULL,
        scratch_shapes=[pltpu.VMEM((n_chip,) + block, F32), pltpu.VMEM((n_chip,) + block, F32), pltpu.VMEM((n_chip,) + block, F32),
                        pltpu.VMEM((n_chip,) + block, F32), pltpu.VMEM((n_sw,) + block, F32),
                        dma((1,)), dma((1,)), dma((n_chip - 1,)), dma((n_chip - 1,)), dma((n_sw - 1,)), dma((n_sw - 1,)),
                        dma((n_chip - 1,)), dma((n_chip - 1,)), dma((1,)), dma((1,))],
        compiler_params=pltpu.CompilerParams(collective_id=cid, has_side_effects=True),
        name=f'sum_all_{cid}',
    )(x)
    return out.reshape(-1)[:size]


def shift_from(strip, axis_name, axis_size, downward):
    if downward:
        perm_pairs = [(i, i + 1) for i in range(axis_size - 1)]
    else:
        perm_pairs = [(i + 1, i) for i in range(axis_size - 1)]
    return lax.ppermute(strip, axis_name, perm_pairs)


def with_halo(dm, flat, grid):
    t = flat.reshape(dm.h, dm.nw, dm.b, dm.cp)
    above = shift_from(t[dm.h - RADIUS:], 'sh', grid[0], True)
    below = shift_from(t[:RADIUS], 'sh', grid[0], False)
    tall = jnp.concatenate([above, t, below], axis=0)
    left = shift_from(tall[:, dm.nw - 1:], 'sw', grid[1], True)
    right = shift_from(tall[:, :1], 'sw', grid[1], False)
    return jnp.concatenate([left, tall, right], axis=1).reshape(-1, dm.cp)


def to_rows(dm, act):
    t = act.reshape(dm.b, dm.h, dm.nw, RADIUS * dm.c).transpose(1, 2, 0, 3)
    return jnp.pad(t, ((0, 0), (0, 0), (0, 0), (0, dm.cp - RADIUS * dm.c))).reshape(dm.rows, dm.cp)


def from_rows(dm, flat):
    t = flat.reshape(dm.h, dm.nw, dm.b, dm.cp)[..., :RADIUS * dm.c].transpose(2, 0, 1, 3)
    return t.reshape(dm.b, dm.h, dm.w, dm.c)


def repeat3(vec, padded):
    t = jnp.concatenate([vec] * 3, axis=-1)
    return jnp.pad(t, [(0, 0)] * (t.ndim - 1) + [(0, padded - t.shape[-1])])


def block_diag(mat, rows, cols):
    r, c = mat.shape
    zero = jnp.zeros((), mat.dtype)
    total = None
    for q in range(3):
        part = lax.pad(mat, zero, ((q * r, rows - (q + 1) * r, 0), (q * c, cols - (q + 1) * c, 0)))
        total = part if total is None else total + part
    return total


def fold_diag(dm, mat, rows, cols):
    return sum(mat[q * rows:(q + 1) * rows, q * cols:(q + 1) * cols] for q in range(3))


def tap_rows(dm, conv_w):
    t = repeat3(conv_w.astype(F32), dm.cp)
    return jnp.pad(t, ((0, 0), (0, 1), (0, 0))).reshape(TAPS * 8, dm.cp)


def constants(dm):
    index = np.arange(dm.cp)
    col, chan = index // dm.c, index % dm.c
    same = (chan[:, None] == chan[None, :]) & (index[:, None] < 3 * dm.c) & (index[None, :] < 3 * dm.c)
    rel = np.where(same, col[:, None] - col[None, :], -100).astype(np.int32)
    ones = ((col[:, None] == col[None, :]) & (index[:, None] < 3 * dm.c) & (index[None, :] < 3 * dm.c)).astype(np.float32)
    return jnp.asarray(rel), ones


def split3(values):
    hi = values.astype(BF16)
    rest = values - hi.astype(F32)
    mid = rest.astype(BF16)
    low = (rest - mid.astype(F32)).astype(BF16)
    return jnp.stack([hi, mid, low])


def params(limit=VMEM_LIMIT):
    return pltpu.CompilerParams(dimension_semantics=('arbitrary',), vmem_limit_bytes=limit)


def call_tiles(dm, th, kernel, tiled, wholes_first, order, outs, scratch, name):
    m = th * dm.rw
    in_specs = []
    for kind, array in order:
        in_specs.append(pl.BlockSpec((m, array.shape[1]), lambda s: (s, 0)) if kind == 't' else FULL)
    out_specs, out_shape = [], []
    for shape, dtype, is_tiled in outs:
        out_shape.append(jax.ShapeDtypeStruct(shape, dtype))
        if is_tiled:
            out_specs.append(pl.BlockSpec((m, shape[1]), lambda s: (s, 0)))
        else:
            out_specs.append(pl.BlockSpec(shape, lambda s, n=len(shape): (0,) * n))
    return pl.pallas_call(kernel, grid=(dm.h // th,), in_specs=in_specs, out_specs=out_specs, out_shape=out_shape,
                          scratch_shapes=scratch, compiler_params=params(), name=name)(*[a for _, a in order])


def solution(mesh):
    grid = (mesh.shape['sh'], mesh.shape['sw'])
    act_spec = P('dp', 'sh', 'sw', None)
    replicated = P()

    def local_step(act_in, drop_mask, grad_out, conv_w, conv_b, norm_g, norm_b, fc1_w, fc1_b, grn_gamma, grn_beta, fc2_w, fc2_b):
        dm = Dims(act_in.shape, fc1_w.shape[-1])
        th = 4
        m = th * dm.rw
        rel, ones32 = constants(dm)
        ones = jnp.asarray(ones32, BF16)
        cvec = lambda v: repeat3(v[None], dm.cp)
        hvec = lambda v: repeat3(v[None], dm.hp)
        cb, ng, nb, b2 = ([cvec(v[k]) for k in range(2)] for v in (conv_b, norm_g, norm_b, fc2_b))
        b1, beta = ([hvec(v[k]) for k in range(2)] for v in (fc1_b, grn_beta))
        gam = [grn_gamma[k][None] for k in range(2)]
        w1 = [block_diag(fc1_w[k], dm.cp, dm.hp) for k in range(2)]
        w1t = [block_diag(fc1_w[k].T, dm.hp, dm.cp) for k in range(2)]
        w2 = [block_diag(fc2_w[k], dm.hp, dm.cp) for k in range(2)]
        w2t = [block_diag(fc2_w[k].T, dm.cp, dm.hp) for k in range(2)]
        taps = [tap_rows(dm, conv_w[k]) for k in range(2)]
        flipped = [tap_rows(dm, conv_w[k, ::-1, ::-1]) for k in range(2)]
        gmat = [split3(jnp.asarray(ones32) * ng[k].reshape(dm.cp, 1)) for k in range(2)]
        masks = [jnp.broadcast_to(drop_mask[:, k:k + 1], (dm.b, dm.cp)) for k in range(2)]

        wide_scr = pltpu.VMEM(((dm.h + 2 * RADIUS) * dm.rw, 3 * dm.cp), BF16)
        toep_scr = pltpu.VMEM((TAPS * 3 * dm.cp, dm.cp), BF16)
        raw_scr = pltpu.VMEM((m, dm.hp), F32)
        hid_scr = pltpu.VMEM((m, dm.hp), BF16)
        c_shape, h_shape, s_shape = (dm.rows, dm.cp), (dm.rows, dm.hp), (dm.b, dm.hp)

        x1 = to_rows(dm, act_in)
        d2 = to_rows(dm, grad_out)

        def forward(k, xp, dout):
            second = k == 1
            order = [('w', xp), ('w', taps[k]), ('w', rel), ('w', cb[k]), ('w', ng[k]), ('w', nb[k]), ('w', ones), ('w', w1[k]), ('w', b1[k])]
            outs = [(c_shape, F32, True), (c_shape, F32, True), (h_shape, BF16, True), (h_shape, F32, True), (s_shape, F32, False)]
            scratch = [wide_scr, toep_scr]
            if second:
                order += [('t', dout), ('w', w2t[k]), ('w', masks[k])]
                outs += [(h_shape, BF16, True), (s_shape, F32, False), (s_shape, F32, False)]
                scratch += [raw_scr]
            return call_tiles(dm, th, functools.partial(forward_kernel, dm, th, second), None, None, order, outs, scratch, f'forward_{k}')

        def backward(k, h, phi, dr, coef, dsq, dout, normed, inv, x=None):
            second = k == 1
            order = [('t', h), ('t', phi), ('t', dr), ('w', coef), ('w', dsq), ('w', beta[k]), ('t', dout), ('w', masks[k]),
                     ('t', normed), ('t', inv), ('w', ng[k]), ('w', nb[k]), ('w', ones), ('w', gmat[k]), ('w', w1t[k])]
            outs = [(c_shape, BF16, True), ((dm.cp, dm.hp), F32, False), ((dm.cp, dm.hp), F32, False), (s_shape, F32, False),
                    ((4, dm.b, dm.cp), F32, False)]
            if second:
                order += [('w', w2[k]), ('w', b2[k]), ('t', x)]
                outs += [(c_shape, BF16, True)]
            return call_tiles(dm, th, functools.partial(backward_kernel, dm, th, second), None, None, order, outs, [hid_scr, hid_scr], f'backward_{k}')

        def input_grad(k, dp, dout, h=None, phi=None):
            last = k == 0
            order = [('w', dp), ('w', flipped[k]), ('w', rel), ('t', dout)]
            outs = [(c_shape, BF16, True)]
            scratch = [wide_scr, toep_scr]
            if not last:
                order += [('w', w2t[0]), ('w', masks[0]), ('t', h), ('t', phi)]
                outs += [(h_shape, BF16, True), (s_shape, F32, False), (s_shape, F32, False)]
                scratch += [raw_scr]
            return call_tiles(dm, th, functools.partial(input_grad_kernel, dm, th, last), None, None, order, outs, scratch, f'input_grad_{k}')

        def wgrad(k, xp, dconv):
            out = pl.pallas_call(
                functools.partial(wgrad_kernel, dm),
                out_shape=jax.ShapeDtypeStruct((TAPS, 8, 3 * dm.cp), F32), in_specs=[FULL] * 3, out_specs=FULL,
                scratch_shapes=[wide_scr, pltpu.VMEM((dm.cp, dm.rows), BF16)],
                compiler_params=pltpu.CompilerParams(vmem_limit_bytes=VMEM_LIMIT), name=f'wgrad_{k}')(xp, dconv, rel)
            t = out[:, :3].reshape(TAPS, 3, 3, dm.cp)[..., :3 * dm.c].reshape(TAPS, 3, 9, dm.c)
            return sum(t[:, q, q:q + TAPS] for q in range(3))

        def small_grads(gfc1, gfc2, sdh, sdr, sums):
            rows = jnp.sum(sums, axis=1)
            csum = sum(rows[:, q * dm.c:(q + 1) * dm.c] for q in range(3))
            hsum = jnp.stack([jnp.sum(sdh, axis=0), jnp.sum(sdr, axis=0)])
            hsum = sum(hsum[:, q * dm.hid:(q + 1) * dm.hid] for q in range(3))
            g1 = fold_diag(dm, gfc1, dm.c, dm.hid)
            g2 = fold_diag(dm, gfc2, dm.c, dm.hid) * np.float32(KEEP)
            return csum, hsum, g1, g2

        xp1 = with_halo(dm, x1, grid)
        normed1, inv1, h1, phi1, ss1 = forward(0, xp1, None)
        norm1, coef1 = grn_reduce(dm, grid, [ss1], [], None, gam[0], 0)
        x2 = call_tiles(dm, th, functools.partial(response_kernel, dm, th), None, None,
                        [('t', h1), ('t', phi1), ('w', coef1), ('w', beta[0]), ('w', w2[0]), ('w', b2[0]), ('t', x1), ('w', masks[0])],
                        [(c_shape, BF16, True)], [hid_scr], 'response')[0]
        xp2 = with_halo(dm, x2, grid)
        normed2, inv2, h2, phi2, ss2, dr2, cross2, sdr2 = forward(1, xp2, d2)
        _, coef2, dsq2, ggam2 = grn_reduce(dm, grid, [ss2], [cross2], None, gam[1], 1)
        dconv2, gfc1_2, gfc2_2, sdh2, sums2, y2 = backward(1, h2, phi2, dr2, coef2, dsq2, d2, normed2, inv2, x2)
        dp2 = with_halo(dm, dconv2, grid)
        gcw2 = wgrad(1, xp2, dconv2)
        d1, dr1, cross1, sdr1 = input_grad(1, dp2, d2, h1, phi1)
        dsq1, ggam1 = grn_reduce(dm, grid, [], [cross1], norm1, gam[0], 2)
        dconv1, gfc1_1, gfc2_1, sdh1, sums1 = backward(0, h1, phi1, dr1, coef1, dsq1, d1, normed1, inv1)
        dp1 = with_halo(dm, dconv1, grid)
        gcw1 = wgrad(0, xp1, dconv1)
        d0 = input_grad(0, dp1, d1)[0]

        per_block = [small_grads(gfc1_1, gfc2_1, sdh1, sdr1, sums1), small_grads(gfc1_2, gfc2_2, sdh2, sdr2, sums2)]
        leaves, tree = jax.tree.flatten((per_block, [gcw1, gcw2]))
        flat = jnp.concatenate([leaf.reshape(-1) for leaf in leaves])
        total = sum_all(grid, flat, 3)
        pieces, start = [], 0
        for leaf in leaves:
            pieces.append(total[start:start + leaf.size].reshape(leaf.shape))
            start += leaf.size
        per_block, gcw = jax.tree.unflatten(tree, pieces)
        csum = jnp.stack([p[0] for p in per_block])
        hsum = jnp.stack([p[1] for p in per_block])
        grads = (jnp.stack(gcw), csum[:, 0], csum[:, 1], csum[:, 2], jnp.stack([p[2] for p in per_block]), hsum[:, 0],
                 jnp.concatenate([ggam1, ggam2]), hsum[:, 1], jnp.stack([p[3].T for p in per_block]), csum[:, 3] * np.float32(KEEP))
        return (from_rows(dm, y2), from_rows(dm, d0)) + grads

    return jax.shard_map(local_step, mesh=mesh,
                         in_specs=(act_spec, P('dp', None), act_spec) + (replicated,) * 10,
                         out_specs=(act_spec, act_spec) + (P('dp'),) * 10,
                         check_vma=False)
```

```python
import functools

import jax
import jax.numpy as jnp
import numpy as np
from jax import lax
from jax.experimental import pallas as pl
from jax.experimental.pallas import tpu as pltpu
from jax.sharding import PartitionSpec as P

EPSILON = 1e-6
RADIUS = 3
TAPS = 2 * RADIUS + 1
MESH = pl.DeviceIdType.MESH
F32 = jnp.float32
BF16 = jnp.bfloat16
KEEP = 4.0 / 3.0
VMEM_LIMIT = 60 * 1024 * 1024
FULL = pl.BlockSpec(memory_space=pltpu.VMEM)
WHOLE = None
CONV_B, NORM_G, NORM_B, FC2_B = range(4)
FC1_B, BETA = range(2)
ONE, TWO = range(2)


def round_up(value, unit):
    return (value + unit - 1) // unit * unit


class Dims:
    def lanes(self, g):
        return slice(g * self.cp, (g + 1) * self.cp)

    def __init__(self, act_shape, hidden):
        self.b, self.h, self.w, self.c = act_shape
        self.hid = hidden
        self.nw = self.w // RADIUS
        self.cp = round_up(RADIUS * self.c, 128)
        self.hp = round_up(RADIUS * hidden, 128)
        self.rw = self.nw * self.b
        self.rows = self.h * self.rw
        self.inner = slice(self.b, self.b + self.rw)
        self.cs = [slice(q * self.c, (q + 1) * self.c) for q in range(RADIUS)]
        self.hs = [slice(q * hidden, (q + 1) * hidden) for q in range(RADIUS)]


def dot(lhs, rhs):
    return jnp.dot(lhs, rhs, preferred_element_type=F32)


def dot_t(lhs, rhs):
    return lax.dot_general(lhs, rhs, (((0,), (0,)), ((), ())), preferred_element_type=F32)


def dot_split(values, rhs):
    hi = values.astype(BF16)
    rest = values - hi.astype(F32)
    mid = rest.astype(BF16)
    low = (rest - mid.astype(F32)).astype(BF16)
    return dot(hi, rhs) + dot(mid, rhs) + dot(low, rhs)


def build_wide(dm, src_ref, wide):

    def body(row, carry):
        block = src_ref[row]
        for g in range(RADIUS):
            wide[pl.ds(pl.multiple_of(row * dm.rw, 16), dm.rw), dm.lanes(g)] = block[g * dm.b:g * dm.b + dm.rw]
        return carry

    lax.fori_loop(0, dm.h + 2 * RADIUS, body, 0)


def build_toeplitz(dm, taps_ref, rel_ref, toep):
    def body(i, carry):
        for g in range(RADIUS):
            acc = jnp.zeros((dm.cp, dm.cp), F32)
            for dj in range(-2, 3):
                j = 3 * g + dj
                if 0 <= j < TAPS:
                    acc = jnp.where(rel_ref[...] == dj, taps_ref[pl.ds(i * 8 + j, 1), :], acc)
            toep[pl.ds(pl.multiple_of((i * 3 + g) * dm.cp, 16), dm.cp), :] = acc.astype(BF16)
        return carry

    lax.fori_loop(0, TAPS, body, 0)


def conv_tile(dm, wide, toep, first_row, th):
    m = th * dm.rw
    acc = None
    for i in range(TAPS):
        rows = pl.ds(pl.multiple_of((first_row + i) * dm.rw, 16), m)
        part = dot(wide[rows, :], toep[i * 3 * dm.cp:(i + 1) * 3 * dm.cp, :])
        acc = part if acc is None else acc + part
    return acc


def lane_loop(dm, th, body):
    def outer(r, carry):
        def inner(lane, c2):
            rows = pl.ds(pl.multiple_of(r * dm.rw, 16), dm.rw)
            body(rows, pl.ds(pl.multiple_of(lane * 128, 128), 128))
            return c2
        return lax.fori_loop(0, dm.hp // 128, inner, carry)
    lax.fori_loop(0, th, outer, 0)


def line(ref, k, row, lanes=slice(None)):
    return ref[k, row:row + 1, lanes]


def image_lines(ref, lanes):
    return ref[:, lanes][None]


def per_image(dm, values):
    return values.reshape(dm.nw, dm.b, values.shape[-1])


def phi_of(hv):
    return 0.5 + 0.5 * lax.erf(hv * np.float32(0.7071067811865476))


def gelu_chunk(dm, h_ref, phi_ref, rows, lanes):
    hv = h_ref[rows, lanes].astype(F32)
    phi = phi_of(hv)
    phi_ref[rows, lanes] = phi
    return hv * phi


def forward_tile(dm, k, th, first, wide, toep, cvec, hvec, ones, w1, normed_o, inv_o, h_o):
    d = (conv_tile(dm, wide, toep, first, th) + line(cvec, k, CONV_B)).astype(BF16)
    mean = dot(d, ones[...]) * np.float32(1.0 / dm.c)
    centered = d.astype(F32) - mean
    var = dot_split(centered * centered, ones[...]) * np.float32(1.0 / dm.c)
    inv = lax.rsqrt(var + EPSILON)
    normed = centered * inv
    normed_o[...] = normed
    inv_o[...] = inv
    n = (normed * line(cvec, k, NORM_G) + line(cvec, k, NORM_B)).astype(BF16)
    h_o[...] = (dot(n, w1[k]) + line(hvec, k, FC1_B)).astype(BF16)


def dot_bt(lhs, rhs):
    return lax.dot_general(lhs, rhs, (((1,), (1,)), ((), ())), preferred_element_type=F32)


def cross_chunk(dm, k, raw, mask, g, dr_o, cross, sdr, rows, lanes):
    dr = (per_image(dm, raw[rows, lanes]) * mask[k, :, :128][None]).astype(BF16)
    dr_o[rows, lanes] = dr.reshape(dm.rw, 128)
    dr32 = dr.astype(F32)
    cross[:, lanes] += jnp.sum(dr32 * per_image(dm, g), axis=0)
    sdr[:, lanes] += jnp.sum(dr32, axis=0)


def position():
    sh = lax.axis_index('sh')
    return sh // 2, sh % 2, lax.axis_index('sw')


def peers_of(grid):
    chip, core, sw = position()
    n_chip, n_sw = grid[0] // 2, grid[1]
    pair = {'sh': chip * 2 + 1 - core}
    row = [{'sh': lax.rem(chip + j, n_chip) * 2 + core} for j in range(1, n_chip)]
    col = [{'sw': lax.rem(sw + j, n_sw)} for j in range(1, n_sw)]
    return pair, row, col


DIRECTIONS = [(0, 1), (0, -1), (1, 0), (-1, 0), (1, 1), (1, -1), (-1, 1), (-1, -1)]


def greet(grid, halo, reduce):
    devices = []
    if halo:
        sh, sw = lax.axis_index('sh'), lax.axis_index('sw')
        for dh, dw in DIRECTIONS:
            devices.append({'sh': lax.rem(sh + dh + grid[0], grid[0]), 'sw': lax.rem(sw + dw + grid[1], grid[1])})
    if reduce:
        pair, row, col = peers_of(grid)
        devices += [pair] + row + col
    barrier = pltpu.get_barrier_semaphore()
    for device in devices:
        pl.semaphore_signal(barrier, inc=1, device_id=device, device_id_type=MESH)
    pl.semaphore_wait(barrier, len(devices))


def clear_halo(dm, xp):
    b, r = dm.b, RADIUS
    edge = (dm.nw + 1) * b
    xp[:r] = jnp.zeros((r,) + xp.shape[1:], BF16)
    xp[dm.h + r:] = jnp.zeros((r,) + xp.shape[1:], BF16)
    xp[r:dm.h + r, :b] = jnp.zeros((dm.h, b, dm.cp), BF16)
    xp[r:dm.h + r, edge:] = jnp.zeros((dm.h, b, dm.cp), BF16)


def halo_copies(dm, grid, xp, send_sem, recv_sem):
    sh, sw = lax.axis_index('sh'), lax.axis_index('sw')
    r, b = RADIUS, dm.b
    rows = {1: (dm.h, r, 0), -1: (r, r, dm.h + r), 0: (r, dm.h, r)}
    cols = {1: (dm.nw * b, b, 0), -1: (b, b, (dm.nw + 1) * b), 0: (b, dm.nw * b, b)}

    def inside(a, c):
        return (a >= 0) & (a < grid[0]) & (c >= 0) & (c < grid[1])

    found = []
    for d, (dh, dw) in enumerate(DIRECTIONS):
        r0, rn, rt = rows[dh]
        c0, cn, ct = cols[dw]
        target = {'sh': lax.rem(sh + dh + grid[0], grid[0]), 'sw': lax.rem(sw + dw + grid[1], grid[1])}
        copy = pltpu.make_async_remote_copy(
            src_ref=xp.at[pl.ds(r0, rn), pl.ds(c0, cn)], dst_ref=xp.at[pl.ds(rt, rn), pl.ds(ct, cn)],
            send_sem=send_sem.at[d], recv_sem=recv_sem.at[d], device_id=target, device_id_type=MESH)
        found.append((copy, inside(sh + dh, sw + dw), inside(sh - dh, sw - dw)))
    return found


def halo_start(copies):
    for copy, sends, _ in copies:
        @pl.when(sends)
        def _():
            copy.start()


def halo_wait(copies):
    for copy, sends, receives in copies:
        @pl.when(sends)
        def _():
            copy.wait_send()

        @pl.when(receives)
        def _():
            copy.wait_recv()


def exchange(slots, mine, devices, send_sem, recv_sem):
    copies = []
    for j, device in enumerate(devices):
        copy = pltpu.make_async_remote_copy(src_ref=slots.at[mine], dst_ref=slots.at[mine], send_sem=send_sem.at[j],
                                            recv_sem=recv_sem.at[j], device_id=device, device_id_type=MESH)
        copies.append(copy)
    return copies


def go(copies):
    for copy in copies:
        copy.start()


def finish(copies):
    for copy in copies:
        copy.wait()


def fold(values, parts):
    return sum(values[:, part] for part in parts)


def sum_slots(slots):
    total = slots[0]
    for j in range(1, slots.shape[0]):
        total = total + slots[j]
    return total


def grn_scratch(dm, grid, count):
    n_chip, n_sw = grid[0] // 2, grid[1]
    dma = pltpu.SemaphoreType.DMA
    block = (count, dm.b, dm.hid)
    return [pltpu.VMEM((2,) + block, F32), pltpu.VMEM((n_chip,) + block, F32), pltpu.VMEM((n_sw,) + block, F32),
            dma((1,)), dma((1,)), dma((n_chip - 1,)), dma((n_chip - 1,)), dma((n_sw - 1,)), dma((n_sw - 1,))]


def grn_total(dm, grid, sums, scratch):
    slots1, slots2, slots3, send1, recv1, send2, recv2, send3, recv3 = scratch
    chip, core, sw = position()
    pair, row, col = peers_of(grid)
    for j, ref in enumerate(sums):
        slots1[core, j] = fold(ref, dm.hs)
    for slots, mine, devices, send, recv, after in ((slots1, core, [pair], send1, recv1, (slots2, chip)),
                                                   (slots2, chip, row, send2, recv2, (slots3, sw)),
                                                   (slots3, sw, col, send3, recv3, WHOLE)):
        copies = exchange(slots, mine, devices, send, recv)
        go(copies)
        finish(copies)
        total = sum_slots(slots)
        if after:
            after[0][after[1]] = total
    return total


def spread(dm, ref, values):
    ref[...] = jnp.zeros_like(ref)
    for part in dm.hs:
        ref[:, part] = values


def grn_cross(dm, norm, gamma, cross, dsq_o, ggam_o):
    mean = jnp.mean(norm, axis=-1, keepdims=True) + EPSILON
    d_scale = gamma * cross
    d_norm = d_scale / mean - jnp.sum(d_scale * norm, axis=-1, keepdims=True) / (mean * mean * dm.hid)
    spread(dm, dsq_o, d_norm / norm)
    ggam_o[...] = jnp.sum(cross * (norm / mean), axis=0, keepdims=True)


def grn_coef(dm, norm, gamma, coef_o):
    mean = jnp.mean(norm, axis=-1, keepdims=True) + EPSILON
    spread(dm, coef_o, gamma * (norm / mean) + 1.0)


def prep_kernel(dm, conv_w, conv_b, norm_g, norm_b, fc1_w, fc1_b, beta, fc2_w, fc2_b, mask_i, ones,
                taps_o, cvec_o, hvec_o, w1_o, w2_o, gmat_o, mask_o):
    for ref in (taps_o, cvec_o, hvec_o, w1_o, w2_o):
        ref[...] = jnp.zeros_like(ref)
    for k in range(2):
        for q in range(RADIUS):
            cs, hs = dm.cs[q], dm.hs[q]
            for i in range(TAPS):
                rows = conv_w[k, i].astype(F32)
                taps_o[k, i * 8:i * 8 + TAPS, cs] = rows
                for j in range(TAPS):
                    taps_o[2 + k, pl.ds((TAPS - 1 - i) * 8 + TAPS - 1 - j, 1), cs] = rows[j:j + 1]
            for j, ref in enumerate((conv_b, norm_g, norm_b, fc2_b)):
                cvec_o[k, j:j + 1, cs] = ref[k:k + 1, :]
            for j, ref in enumerate((fc1_b, beta)):
                hvec_o[k, j:j + 1, hs] = ref[k:k + 1, :]
            w1_o[k, cs, hs] = fc1_w[k]
            w2_o[k, hs, cs] = fc2_w[k]
        mask_o[k] = jnp.broadcast_to(mask_i[:, k:k + 1], (dm.b, dm.cp))
    for k in range(2):
        values = ones[...].astype(F32) * line(cvec_o, k, NORM_G)
        for j in range(RADIUS):
            part = values.astype(BF16)
            gmat_o[k, j] = part
            values = values - part.astype(F32)


def first_kernel(dm, grid, th, x, taps, rel, cvec, hvec, ones, w1, gamma,
                 normed_o, inv_o, h_o, phi_o, xp_o, norm_o, coef_o, wide, toep, ss, xp, keep_sem, send, recv, *grn):
    step = pl.program_id(0)

    @pl.when(step == 0)
    def _():
        clear_halo(dm, xp)
        for row in range(dm.h):
            xp[row + RADIUS, dm.inner] = x[row * dm.rw:(row + 1) * dm.rw]
        greet(grid, True, True)
        copies = halo_copies(dm, grid, xp, send, recv)
        halo_start(copies)
        build_toeplitz(dm, taps.at[0], rel, toep)
        ss[...] = jnp.zeros_like(ss)
        halo_wait(copies)
        pltpu.make_async_copy(xp, xp_o, keep_sem).start()
        build_wide(dm, xp, wide)

    forward_tile(dm, 0, th, step * th, wide, toep, cvec, hvec, ones, w1, normed_o, inv_o, h_o)

    def body(rows, lanes):
        g = gelu_chunk(dm, h_o, phi_o, rows, lanes)
        ss[:, lanes] += jnp.sum(per_image(dm, g * g), axis=0)

    lane_loop(dm, th, body)

    @pl.when(step == pl.num_programs(0) - 1)
    def _():
        pltpu.make_async_copy(xp, xp_o, keep_sem).wait()
        norm = jnp.sqrt(grn_total(dm, grid, [ss], grn)[0])
        norm_o[...] = norm
        grn_coef(dm, norm, gamma[pl.ds(ONE, 1), :], coef_o)


def second_kernel(dm, grid, th, h1, phi1, x1, coef1, taps, rel, cvec, hvec, ones, w1, w2, gamma, mask, dout,
                  normed_o, inv_o, h_o, phi_o, dr_o, xp_o, sdr_o, coef_o, dsq_o, ggam_o,
                  wide, toep, resp, raw, ss, cross, xp, keep_sem, send, recv, *grn):
    step = pl.program_id(0)
    tiles = dm.h // th

    @pl.when(step == 0)
    def _():
        clear_halo(dm, xp)
        greet(grid, True, True)
        for ref in (ss, cross, sdr_o):
            ref[...] = jnp.zeros_like(ref)

    @pl.when(step < tiles)
    def _():
        def body(rows, lanes):
            g = h1[rows, lanes].astype(F32) * phi1[rows, lanes]
            r = per_image(dm, g) * image_lines(coef1, lanes) + line(hvec, ONE, BETA, lanes)
            resp[rows, lanes] = r.reshape(dm.rw, 128).astype(BF16)

        lane_loop(dm, th, body)
        o = (dot(resp[...], w2[ONE]) + line(cvec, ONE, FC2_B)).reshape(-1, dm.b, dm.cp)
        y = (x1[...].astype(F32) + (o * mask[ONE][None]).reshape(-1, dm.cp)).astype(BF16)
        for r in range(th):
            xp[step * th + r + RADIUS, dm.inner] = y[r * dm.rw:(r + 1) * dm.rw]

    @pl.when(step == tiles)
    def _():
        copies = halo_copies(dm, grid, xp, send, recv)
        halo_start(copies)
        build_toeplitz(dm, taps.at[1], rel, toep)
        halo_wait(copies)
        pltpu.make_async_copy(xp, xp_o, keep_sem).start()
        build_wide(dm, xp, wide)

    @pl.when(step >= tiles)
    def _():
        forward_tile(dm, 1, th, (step - tiles) * th, wide, toep, cvec, hvec, ones, w1, normed_o, inv_o, h_o)
        raw[...] = dot_bt(dout[...], w2[TWO])

        def body(rows, lanes):
            g = gelu_chunk(dm, h_o, phi_o, rows, lanes)
            ss[:, lanes] += jnp.sum(per_image(dm, g * g), axis=0)
            cross_chunk(dm, 1, raw, mask, g, dr_o, cross, sdr_o, rows, lanes)

        lane_loop(dm, th, body)

    @pl.when(step == pl.num_programs(0) - 1)
    def _():
        pltpu.make_async_copy(xp, xp_o, keep_sem).wait()
        total = grn_total(dm, grid, [ss, cross], grn)
        norm = jnp.sqrt(total[0])
        grn_coef(dm, norm, gamma[pl.ds(TWO, 1), :], coef_o)
        grn_cross(dm, norm, gamma[pl.ds(TWO, 1), :], total[1], dsq_o, ggam_o)


def backward_tile(dm, k, h_i, phi_i, dr_i, coef, dsq, dout, normed_i, inv_i, cvec, hvec, ones, gmat, w1, w2, mask,
                  resp, dh, gfc1, gfc2, sdh, sums, th, x_rows, y_o):
    def body(rows, lanes):
        hv = h_i[rows, lanes].astype(F32)
        phi = phi_i[rows, lanes]
        g = per_image(dm, hv * phi)
        a = image_lines(coef, lanes)
        resp[rows, lanes] = (g * a + line(hvec, k, BETA, lanes)).reshape(dm.rw, 128).astype(BF16)
        slope = phi + hv * (np.float32(0.3989422804014327) * jnp.exp(-0.5 * hv * hv))
        dg = per_image(dm, dr_i[rows, lanes].astype(F32)) * a + g * image_lines(dsq, lanes)
        dhv = (dg.reshape(dm.rw, 128) * slope).astype(BF16)
        dh[rows, lanes] = dhv
        sdh[:, lanes] += jnp.sum(per_image(dm, dhv.astype(F32)), axis=0)

    lane_loop(dm, th, body)
    dsel32 = jnp.where((mask[k] != 0.0)[None], dout[...].astype(F32).reshape(-1, dm.b, dm.cp), 0.0)
    sums[FC2_B] += jnp.sum(dsel32, axis=0)
    gfc2[...] += dot_t(dsel32.reshape(-1, dm.cp).astype(BF16), resp[...])
    if y_o is not None:
        o = (dot(resp[...], w2[k]) + line(cvec, k, FC2_B)).reshape(-1, dm.b, dm.cp)
        y_o[...] = (x_rows.astype(F32) + (o * mask[k][None]).reshape(-1, dm.cp)).astype(BF16)
    normed = normed_i[...]
    norm_g = line(cvec, k, NORM_G)
    n = (normed * norm_g + line(cvec, k, NORM_B)).astype(BF16)
    gfc1[...] += dot_t(n, dh[...])
    dn16 = dot_bt(dh[...], w1[k]).astype(BF16)
    dn = dn16.astype(F32)
    scale = np.float32(1.0 / dm.c)
    mean1 = (dot_bt(dn16, gmat[k, 0]) + dot_bt(dn16, gmat[k, 1]) + dot_bt(dn16, gmat[k, 2])) * scale
    dnormed = dn * norm_g
    mean2 = dot_split(dnormed * normed, ones[...]) * scale
    dconv = (inv_i[...] * (dnormed - mean1 - normed * mean2)).astype(BF16)

    for row, values in ((CONV_B, dconv.astype(F32)), (NORM_G, dn * normed), (NORM_B, dn)):
        sums[row] += jnp.sum(values.reshape(-1, dm.b, dm.cp), axis=0)
    return dconv


def wgrad(dm, wide, dcol, rel, out):
    keep = rel[...] > -50

    def body(i, carry):
        rows = pl.ds(pl.multiple_of(i * dm.rw, 16), dm.rows)
        res = dot(dcol[...], wide[rows, :])
        for g in range(RADIUS):
            part = jnp.where(keep, res[:, dm.lanes(g)], 0.0)
            for q in range(RADIUS):
                out[q, pl.ds(i, 1), dm.lanes(g)] = jnp.sum(part[dm.cs[q]], axis=0, keepdims=True)
        return carry

    lax.fori_loop(0, TAPS, body, 0)


PACK_ROWS = 256


def pack_grads(dm, pack, gfc1, gfc2, corr, sdh, sdr, sums):
    c, hid = dm.c, dm.hid
    for base, ref in ((0, gfc1), (c, gfc2)):
        pack[base:base + c, :hid] = sum(ref[cs, hs] for cs, hs in zip(dm.cs, dm.hs))
    base = 2 * c
    for j in range(TAPS):
        total = None
        for q in range(RADIUS):
            p = q + j
            lane = (p // 3) * dm.cp + (p % 3) * c
            part = corr[q, :, lane:lane + c]
            total = part if total is None else total + part
        pack[base + 8 * j:base + 8 * j + 8, :c] = total
    base += 8 * TAPS
    for row, ref in enumerate((sdh, sdr)):
        vec = jnp.sum(ref[...], axis=0, keepdims=True)
        pack[base + row:base + row + 1, :hid] = fold(vec, dm.hs)
    for row in range(4):
        vec = jnp.sum(sums[row], axis=0, keepdims=True)
        pack[base + 2 + row:base + 3 + row, :c] = fold(vec, dm.cs)


def pack_shape(dm, grid):
    return (PACK_ROWS, round_up(dm.hid, 128))


def sum_scratch(dm, grid):
    rows, lanes = pack_shape(dm, grid)
    n_chip, n_sw = grid[0] // 2, grid[1]
    half, chunk = rows // 2, rows // (2 * n_chip)
    dma = pltpu.SemaphoreType.DMA
    return [pltpu.VMEM((half, lanes), F32), pltpu.VMEM((n_chip, chunk, lanes), F32), pltpu.VMEM((n_chip, chunk, lanes), F32),
            pltpu.VMEM((n_chip, chunk, lanes), F32), pltpu.VMEM((n_sw, chunk, lanes), F32),
            dma((1,)), dma((1,)), dma((n_chip - 1,)), dma((n_chip - 1,)), dma((n_sw - 1,)), dma((n_sw - 1,)),
            dma((n_chip - 1,)), dma((n_chip - 1,)), dma((1,)), dma((1,))]


N_SUM = 15


def sum_stages(grid, x, out, scratch):
    got1, half, got2, part, slots3, send1, recv1, send2, recv2, send3, recv3, send4, recv4, send5, recv5 = scratch
    chip, core, sw = position()
    n_chip = grid[0] // 2
    pair, row, col = peers_of(grid)
    rows = got1.shape[0]
    chunk = half.shape[1]

    def whole(ref, which):
        return ref.at[pl.ds(pl.multiple_of(which * rows, 8), rows)]

    def copies1():
        return [pltpu.make_async_remote_copy(src_ref=whole(x, 1 - core), dst_ref=got1, send_sem=send1.at[0], recv_sem=recv1.at[0],
                                             device_id=pair, device_id_type=MESH)]

    def copies2():
        made = []
        for j, device in enumerate(row):
            made.append(pltpu.make_async_remote_copy(
                src_ref=half.at[lax.rem(chip + j + 1, n_chip)], dst_ref=got2.at[chip], send_sem=send2.at[j],
                recv_sem=recv2.at[j], device_id=device, device_id_type=MESH))
        return made

    def copies5():
        return [pltpu.make_async_remote_copy(src_ref=whole(out, core), dst_ref=whole(out, core), send_sem=send5.at[0],
                                             recv_sem=recv5.at[0], device_id=pair, device_id_type=MESH)]

    def stage0():
        go(copies1())

    def stage1():
        finish(copies1())
        for j in range(n_chip):
            start = pl.multiple_of(core * rows + j * chunk, 8)
            half[j] = x[pl.ds(start, chunk)] + got1[j * chunk:(j + 1) * chunk]
        go(copies2())

    def stage2():
        got2[chip] = half[chip]
        finish(copies2())
        slots3[sw] = sum_slots(got2)
        go(exchange(slots3, sw, col, send3, recv3))

    def stage3():
        finish(exchange(slots3, sw, col, send3, recv3))
        part[chip] = sum_slots(slots3)
        go(exchange(part, chip, row, send4, recv4))

    def stage4():
        finish(exchange(part, chip, row, send4, recv4))
        for j in range(n_chip):
            out[pl.ds(pl.multiple_of(core * rows + j * chunk, 8), chunk)] = part[j]
        go(copies5())

    def stage5():
        finish(copies5())

    return [stage0, stage1, stage2, stage3, stage4, stage5]


def third_kernel(dm, grid, th, h2, phi2, dr2, coef2, dsq2, dout, normed, inv, xp2, h1, phi1, norm1, taps, rel, cvec, hvec, ones, gmat,
                 w1, w2, gamma, mask, sdr2,
                 y_o, d1_o, dr1_o, pack, sdr_o, dsq_o, ggam_o,
                 wide, toep, dp, dcol, corr, resp, dh, raw, gfc1, gfc2, sdh, sums, cross, send, recv, *grn):
    step = pl.program_id(0)
    tiles = dm.h // th

    @pl.when(step == 0)
    def _():
        clear_halo(dm, dp)
        greet(grid, True, True)
        build_wide(dm, xp2, wide)
        for ref in (cross, sdr_o, gfc1, gfc2, sdh, sums, corr, pack):
            ref[...] = jnp.zeros_like(ref)

    @pl.when(step < tiles)
    def _():
        x_rows = jnp.concatenate([xp2[step * th + r + RADIUS, dm.inner] for r in range(th)], axis=0)
        dconv = backward_tile(dm, 1, h2, phi2, dr2, coef2, dsq2, dout, normed, inv, cvec, hvec, ones, gmat, w1, w2, mask,
                              resp, dh, gfc1, gfc2, sdh, sums, th, x_rows, y_o)
        for r in range(th):
            dp[step * th + r + RADIUS, dm.inner] = dconv[r * dm.rw:(r + 1) * dm.rw]
        for j in range(tiles):
            @pl.when(step == j)
            def _():
                dcol[:, j * th * dm.rw:(j + 1) * th * dm.rw] = dconv.T

    @pl.when(step == tiles)
    def _():
        copies = halo_copies(dm, grid, dp, send, recv)
        halo_start(copies)
        build_toeplitz(dm, taps.at[3], rel, toep)
        wgrad(dm, wide, dcol, rel, corr)
        pack_grads(dm, pack, gfc1, gfc2, corr, sdh, sdr2, sums)
        halo_wait(copies)
        build_wide(dm, dp, wide)

    @pl.when(step >= tiles)
    def _():
        din = (dout[...].astype(F32) + conv_tile(dm, wide, toep, (step - tiles) * th, th)).astype(BF16)
        d1_o[...] = din
        raw[...] = dot_bt(din, w2[ONE])

        def body(rows, lanes):
            g = h1[rows, lanes].astype(F32) * phi1[rows, lanes]
            cross_chunk(dm, 0, raw, mask, g, dr1_o, cross, sdr_o, rows, lanes)

        lane_loop(dm, th, body)

    @pl.when(step == pl.num_programs(0) - 1)
    def _():
        total = grn_total(dm, grid, [cross], grn)
        grn_cross(dm, norm1[...], gamma[pl.ds(ONE, 1), :], total[0], dsq_o, ggam_o)


def fourth_kernel(dm, grid, th, h1, phi1, dr1, coef1, dsq1, d1, normed, inv, xp1, taps, rel, cvec, hvec, ones, gmat,
                  w1, w2, mask, sdr1, pack2_i,
                  d0_o, out1_o, out2_o,
                  wide, toep, dp, dcol, corr, resp, dh, gfc1, gfc2, sdh, sums, pack1, pack2, out1, out2, send, recv, *sem):
    step = pl.program_id(0)
    tiles = dm.h // th
    stages1 = sum_stages(grid, pack1, out1, sem[:N_SUM])
    stages2 = sum_stages(grid, pack2, out2, sem[N_SUM:])

    @pl.when(step == 0)
    def _():
        clear_halo(dm, dp)
        greet(grid, True, True)
        for ref in (gfc1, gfc2, sdh, sums, corr, pack1):
            ref[...] = jnp.zeros_like(ref)
        pack2[...] = pack2_i[...]

    for j in range(6):
        @pl.when(step == j)
        def _():
            stages2[j]()

        @pl.when(step == tiles + j)
        def _():
            if 0 < j < 5:
                stages1[j - 1]()

    @pl.when(step == 0)
    def _():
        build_wide(dm, xp1, wide)

    @pl.when(step < tiles)
    def _():
        dconv = backward_tile(dm, 0, h1, phi1, dr1, coef1, dsq1, d1, normed, inv, cvec, hvec, ones, gmat, w1, w2, mask,
                              resp, dh, gfc1, gfc2, sdh, sums, th, None, WHOLE)
        for r in range(th):
            dp[step * th + r + RADIUS, dm.inner] = dconv[r * dm.rw:(r + 1) * dm.rw]
        for j in range(tiles):
            @pl.when(step == j)
            def _():
                dcol[:, j * th * dm.rw:(j + 1) * th * dm.rw] = dconv.T

    @pl.when(step == tiles)
    def _():
        copies = halo_copies(dm, grid, dp, send, recv)
        halo_start(copies)
        build_toeplitz(dm, taps.at[2], rel, toep)
        wgrad(dm, wide, dcol, rel, corr)
        pack_grads(dm, pack1, gfc1, gfc2, corr, sdh, sdr1, sums)
        halo_wait(copies)
        build_wide(dm, dp, wide)

    @pl.when(step >= tiles)
    def _():
        din = (d1[...].astype(F32) + conv_tile(dm, wide, toep, (step - tiles) * th, th)).astype(BF16)
        d0_o[...] = din

    @pl.when(step == pl.num_programs(0) - 1)
    def _():
        stages1[4]()
        stages1[5]()
        out1_o[...] = out1[...]
        out2_o[...] = out2[...]


def final_kernel(dm, out1, out2, ggam1, ggam2, gcw, gcb, gng, gnb, gf1w, gf1b, ggam, gbeta, gf2w, gf2b):
    c, hid = dm.c, dm.hid
    ggam[...] = jnp.concatenate([ggam1[...], ggam2[...]], axis=0)
    for k, ref in enumerate((out1, out2)):
        gf1w[k] = ref[:c, :hid]
        gf2w[k] = ref[c:2 * c, :hid].T * np.float32(KEEP)
        base = 2 * c
        for j in range(TAPS):
            for i in range(TAPS):
                gcw[k, i, j:j + 1, :] = ref[base + 8 * j + i:base + 8 * j + i + 1, :c]
        base += 8 * TAPS
        for row, out in enumerate((gf1b, gbeta, gcb, gng, gnb, gf2b)):
            value = ref[base + row:base + row + 1, :out.shape[1]]
            out[k:k + 1, :] = value * np.float32(KEEP) if out is gf2b else value


def to_rows(dm, act):
    t = act.reshape(dm.b, dm.h, dm.nw, RADIUS * dm.c).transpose(1, 2, 0, 3)
    return jnp.pad(t, ((0, 0), (0, 0), (0, 0), (0, dm.cp - RADIUS * dm.c))).reshape(dm.rows, dm.cp)


def from_rows(dm, flat):
    t = flat.reshape(dm.h, dm.nw, dm.b, dm.cp)[..., :RADIUS * dm.c].transpose(2, 0, 1, 3)
    return t.reshape(dm.b, dm.h, dm.w, dm.c)


def constants(dm):
    index = np.arange(dm.cp)
    col, chan = index // dm.c, index % dm.c
    live = (index[:, None] < RADIUS * dm.c) & (index[None, :] < RADIUS * dm.c)
    rel = np.where((chan[:, None] == chan[None, :]) & live, col[:, None] - col[None, :], -100).astype(np.int32)
    ones = ((col[:, None] == col[None, :]) & live).astype(np.float32)
    return jnp.asarray(rel), jnp.asarray(ones, BF16)


def call(dm, th, kernel, steps, ins, outs, scratch, name, cid=None):
    m, tiles = th * dm.rw, dm.h // th

    def spec(shape, first):
        if first is None:
            return FULL
        if first == 'any':
            return pl.BlockSpec(memory_space=pl.ANY)
        if first == 'both':
            return pl.BlockSpec((m, shape[1]), lambda s: (lax.rem(s, tiles), 0))
        return pl.BlockSpec((m, shape[1]), lambda s: (jnp.clip(s - first, 0, tiles - 1), 0))

    return pl.pallas_call(
        kernel, grid=(steps,), in_specs=[spec(a.shape, first) for a, first in ins],
        out_specs=[spec(shape, first) for shape, _, first in outs],
        out_shape=[jax.ShapeDtypeStruct(shape, dtype) for shape, dtype, _ in outs],
        scratch_shapes=scratch, name=name,
        compiler_params=pltpu.CompilerParams(dimension_semantics=('arbitrary',), vmem_limit_bytes=VMEM_LIMIT,
                                             collective_id=cid, has_side_effects=True))(*[a for a, _ in ins])


def solution(mesh):
    grid = (mesh.shape['sh'], mesh.shape['sw'])
    act_spec = P('dp', 'sh', 'sw', WHOLE)
    replicated = P()

    def local_step(act_in, drop_mask, grad_out, conv_w, conv_b, norm_g, norm_b, fc1_w, fc1_b, gamma, grn_beta, fc2_w, fc2_b):
        dm = Dims(act_in.shape, fc1_w.shape[-1])
        th = 4
        tiles, m = dm.h // th, th * dm.rw
        rel, ones = constants(dm)
        sds = jax.ShapeDtypeStruct
        taps, cvec, hvec, w1, w2, gmat, mask = pl.pallas_call(
            functools.partial(prep_kernel, dm),
            out_shape=[sds((4, TAPS * 8, dm.cp), F32), sds((2, 4, dm.cp), F32), sds((2, 2, dm.hp), F32), sds((2, dm.cp, dm.hp), BF16),
                       sds((2, dm.hp, dm.cp), BF16), sds((2, 3, dm.cp, dm.cp), BF16), sds((2, dm.b, dm.cp), F32)],
            in_specs=[FULL] * 11, out_specs=[FULL] * 7, name='prep')(
                conv_w, conv_b, norm_g, norm_b, fc1_w, fc1_b, grn_beta, fc2_w, fc2_b, drop_mask, ones)

        dma = pltpu.SemaphoreType.DMA
        V = pltpu.VMEM
        wide_s = V(((dm.h + 2 * RADIUS) * dm.rw, 3 * dm.cp), BF16)
        toep_s = V((TAPS * 3 * dm.cp, dm.cp), BF16)
        raw_s, hid_s = V((m, dm.hp), F32), V((m, dm.hp), BF16)
        img_s = V((dm.b, dm.hp), F32)
        acc_s = V((dm.cp, dm.hp), F32)
        xp_shape = (dm.h + 2 * RADIUS, (dm.nw + 2) * dm.b, dm.cp)
        halo_s = [dma((8,)), dma((8,))]
        c_shape, h_shape, s_shape, n_shape = (dm.rows, dm.cp), (dm.rows, dm.hp), (dm.b, dm.hp), (dm.b, dm.hid)
        g_shape = (1, dm.hid)
        p_shape = pack_shape(dm, grid)

        x1 = to_rows(dm, act_in)
        d2 = to_rows(dm, grad_out)

        normed1, inv1, h1, phi1, xp1, norm1, coef1 = call(
            dm, th, functools.partial(first_kernel, dm, grid, th), tiles,
            [(a, WHOLE) for a in (x1, taps, rel, cvec, hvec, ones, w1, gamma)],
            [(c_shape, F32, 0), (c_shape, F32, 0), (h_shape, BF16, 0), (h_shape, F32, 0), (xp_shape, BF16, 'any'), (n_shape, F32, WHOLE),
             (s_shape, F32, WHOLE)],
            [wide_s, toep_s, img_s, V(xp_shape, BF16), dma] + halo_s + grn_scratch(dm, grid, 1), 'first', 0)

        normed2, inv2, h2, phi2, dr2, xp2, sdr2, coef2, dsq2, ggam2 = call(
            dm, th, functools.partial(second_kernel, dm, grid, th), 2 * tiles,
            [(h1, 0), (phi1, 0), (x1, 0), (coef1, WHOLE)] + [(a, WHOLE) for a in (taps, rel, cvec, hvec, ones, w1, w2, gamma, mask)]
            + [(d2, tiles)],
            [(c_shape, F32, tiles), (c_shape, F32, tiles), (h_shape, BF16, tiles), (h_shape, F32, tiles), (h_shape, BF16, tiles),
             (xp_shape, BF16, 'any'), (s_shape, F32, WHOLE), (s_shape, F32, WHOLE), (s_shape, F32, WHOLE), (g_shape, F32, WHOLE)],
            [wide_s, toep_s, hid_s, raw_s, img_s, img_s, V(xp_shape, BF16), dma] + halo_s + grn_scratch(dm, grid, 2), 'second', 1)

        bwd_s = [wide_s, toep_s, V(xp_shape, BF16), V((dm.cp, dm.rows), BF16), V((3, 8, 3 * dm.cp), F32), hid_s, hid_s]
        acc = [acc_s, acc_s, img_s, V((4, dm.b, dm.cp), F32)]
        y2, d1, dr1, pack2, sdr1, dsq1, ggam1 = call(
            dm, th, functools.partial(third_kernel, dm, grid, th), 2 * tiles,
            [(h2, 0), (phi2, 0), (dr2, 0), (coef2, WHOLE), (dsq2, WHOLE), (d2, 'both'), (normed2, 0), (inv2, 0), (xp2, WHOLE),
             (h1, tiles), (phi1, tiles)] + [(a, WHOLE) for a in (norm1, taps, rel, cvec, hvec, ones, gmat, w1, w2, gamma, mask, sdr2)],
            [(c_shape, BF16, 0), (c_shape, BF16, tiles), (h_shape, BF16, tiles), (p_shape, F32, WHOLE), (s_shape, F32, WHOLE),
             (s_shape, F32, WHOLE), (g_shape, F32, WHOLE)],
            bwd_s + [raw_s] + acc + [img_s] + halo_s + grn_scratch(dm, grid, 1), 'third', 2)

        d0, out1, out2 = call(
            dm, th, functools.partial(fourth_kernel, dm, grid, th), 2 * tiles,
            [(h1, 0), (phi1, 0), (dr1, 0), (coef1, WHOLE), (dsq1, WHOLE), (d1, 'both'), (normed1, 0), (inv1, 0), (xp1, WHOLE)]
            + [(a, WHOLE) for a in (taps, rel, cvec, hvec, ones, gmat, w1, w2, mask, sdr1, pack2)],
            [(c_shape, BF16, tiles), (p_shape, F32, WHOLE), (p_shape, F32, WHOLE)],
            bwd_s + acc + [V(p_shape, F32)] * 4 + halo_s + sum_scratch(dm, grid) * 2, 'fourth', 3)

        grads = pl.pallas_call(
            functools.partial(final_kernel, dm),
            out_shape=[sds(s, F32) for s in (conv_w.shape, conv_b.shape, norm_g.shape, norm_b.shape, fc1_w.shape, fc1_b.shape, gamma.shape,
                                             grn_beta.shape, fc2_w.shape, fc2_b.shape)],
            in_specs=[FULL] * 4, out_specs=[FULL] * 10, name='final')(out1, out2, ggam1, ggam2)
        return (from_rows(dm, y2), from_rows(dm, d0)) + tuple(grads)

    return jax.shard_map(local_step, mesh=mesh,
                         in_specs=(act_spec, P('dp', WHOLE), act_spec) + (replicated,) * 10,
                         out_specs=(act_spec, act_spec) + (P('dp'),) * 10,
                         check_vma=False)
```

```python
import functools

import jax
import jax.numpy as jnp
import numpy as np
from jax import lax
from jax.experimental import pallas as pl
from jax.experimental.pallas import tpu as pltpu
from jax.sharding import PartitionSpec as P

EPSILON = 1e-6
RADIUS = 3
TAPS = 2 * RADIUS + 1
MESH = pl.DeviceIdType.MESH
F32 = jnp.float32
BF16 = jnp.bfloat16
KEEP = 4.0 / 3.0
VMEM_LIMIT = 60 * 1024 * 1024
FULL = pl.BlockSpec(memory_space=pltpu.VMEM)
WHOLE = None
CONV_B, NORM_G, NORM_B, FC2_B = range(4)
FC1_B, BETA = range(2)
ONE, TWO = range(2)


def round_up(value, unit):
    return (value + unit - 1) // unit * unit


class Dims:
    def lanes(self, g):
        return slice(g * self.cp, (g + 1) * self.cp)

    def __init__(self, act_shape, hidden):
        self.b, self.h, self.w, self.c = act_shape
        self.hid = hidden
        self.nw = self.w // RADIUS
        self.cp = round_up(RADIUS * self.c, 128)
        self.hp = round_up(RADIUS * hidden, 128)
        self.pairs = ((1, 2), (0, self.nw - 1))
        self.rw = 2 * self.b
        self.chunk = 2 * self.rw
        self.th = self.h // RADIUS
        self.half = RADIUS
        self.tiles = 2 * self.half
        self.m = self.th * self.rw
        self.rows = self.h * self.nw * self.b
        self.block = self.h * self.rw
        self.tall = (self.h + 2 * RADIUS) * self.rw
        self.inner = slice(self.b, self.b + self.nw * self.b)
        self.cs = [slice(q * self.c, (q + 1) * self.c) for q in range(RADIUS)]
        self.hs = [slice(q * hidden, (q + 1) * hidden) for q in range(RADIUS)]


def loop(count, body, init=0):
    return lax.fori_loop(0, count, body, init)


def dot(lhs, rhs):
    return jnp.dot(lhs, rhs, preferred_element_type=F32)


def dot_t(lhs, rhs):
    return lax.dot_general(lhs, rhs, (((0,), (0,)), ((), ())), preferred_element_type=F32)


def dot_split(values, rhs):
    hi = values.astype(BF16)
    rest = values - hi.astype(F32)
    mid = rest.astype(BF16)
    low = (rest - mid.astype(F32)).astype(BF16)
    return dot(hi, rhs) + dot(mid, rhs) + dot(low, rhs)


def build_wide(dm, src_ref, wide, pair):
    def body(row, carry):
        rows = pl.ds(pl.multiple_of(pair * dm.tall + row * dm.rw, 16), dm.rw)
        for g in range(RADIUS):
            parts = [src_ref[row, (wg + g) * dm.b:(wg + g + 1) * dm.b] for wg in dm.pairs[pair]]
            wide[rows, dm.lanes(g)] = jnp.concatenate(parts, axis=0)
        return carry

    loop(dm.h + 2 * RADIUS, body)


def each_part(dm, tile, col0, body):
    row0 = lax.rem(tile, dm.half) * dm.th
    for pair, groups in enumerate(dm.pairs):
        @pl.when(tile // dm.half == pair)
        def _():
            for r in range(dm.th):
                for j, wg in enumerate(groups):
                    at, col = r * dm.rw + j * dm.b, col0 + wg * dm.b
                    body(slice(at, at + dm.b), row0 + r, slice(col, col + dm.b))


def load_tile(dm, ref, tile_ref, tile, col0, row_off):
    def body(part, row, cols):
        tile_ref[part] = ref[row + row_off, cols]

    each_part(dm, tile, col0, body)


def store_tile(dm, ref, values, tile, col0, row_off):
    def body(part, row, cols):
        ref[row + row_off, cols] = values[part]

    each_part(dm, tile, col0, body)


def build_toeplitz(dm, taps_ref, rel_ref, toep):
    def body(i, carry):
        for g in range(RADIUS):
            acc = jnp.zeros((dm.cp, dm.cp), F32)
            for dj in range(-2, 3):
                j = 3 * g + dj
                if 0 <= j < TAPS:
                    acc = jnp.where(rel_ref[...] == dj, taps_ref[pl.ds(i * 8 + j, 1), :], acc)
            toep[pl.ds(pl.multiple_of((i * 3 + g) * dm.cp, 16), dm.cp), :] = acc.astype(BF16)
        return carry

    loop(TAPS, body)


def conv_tile(dm, wide, toep, tile):
    base = (tile // dm.half) * dm.tall + lax.rem(tile, dm.half) * dm.m
    acc = None
    for i in range(TAPS):
        rows = pl.ds(pl.multiple_of(base + i * dm.rw, 16), dm.m)
        part = dot(wide[rows, :], toep[i * 3 * dm.cp:(i + 1) * 3 * dm.cp, :])
        acc = part if acc is None else acc + part
    return acc


def lane_loop(dm, body):
    def outer(r, carry):
        def inner(lane, c2):
            body(pl.ds(pl.multiple_of(r * dm.chunk, 16), dm.chunk), pl.ds(pl.multiple_of(lane * 128, 128), 128))
            return c2
        return loop(dm.hp // 128, inner, carry)
    loop(dm.m // dm.chunk, outer)


def line(ref, k, row, lanes=slice(None)):
    return ref[k, row:row + 1, lanes]


def image_lines(ref, lanes):
    return ref[:, lanes][None]


def per_image(dm, values):
    return values.reshape(-1, dm.b, values.shape[-1])


def phi_of(hv):
    return 0.5 + 0.5 * lax.erf(hv * np.float32(0.7071067811865476))


def gelu_chunk(dm, h_ref, phi_ref, rows, lanes):
    hv = h_ref[rows, lanes].astype(F32)
    phi = phi_of(hv)
    phi_ref[rows, lanes] = phi
    return hv * phi


def forward_tile(dm, k, tile, wide, toep, cvec, hvec, ones, w1, normed_o, inv_o, h_o):
    d = (conv_tile(dm, wide, toep, tile) + line(cvec, k, CONV_B)).astype(BF16)
    mean = dot(d, ones[...]) * np.float32(1.0 / dm.c)
    centered = d.astype(F32) - mean
    var = dot_split(centered * centered, ones[...]) * np.float32(1.0 / dm.c)
    inv = lax.rsqrt(var + EPSILON)
    normed = centered * inv
    normed_o[...] = normed
    inv_o[...] = inv
    n = (normed * line(cvec, k, NORM_G) + line(cvec, k, NORM_B)).astype(BF16)
    h_o[...] = (dot(n, w1[k]) + line(hvec, k, FC1_B)).astype(BF16)


def dot_bt(lhs, rhs):
    return lax.dot_general(lhs, rhs, (((1,), (1,)), ((), ())), preferred_element_type=F32)


def cross_chunk(dm, k, raw, mask, g, dr_o, cross, sdr, rows, lanes):
    dr = (per_image(dm, raw[rows, lanes]) * mask[k, :, :128][None]).astype(BF16)
    dr_o[rows, lanes] = dr.reshape(dm.chunk, 128)
    dr32 = dr.astype(F32)
    cross[:, lanes] += jnp.sum(dr32 * per_image(dm, g), axis=0)
    sdr[:, lanes] += jnp.sum(dr32, axis=0)


def position():
    sh = lax.axis_index('sh')
    return sh // 2, sh % 2, lax.axis_index('sw')


def peers_of(grid):
    chip, core, sw = position()
    n_chip, n_sw = grid[0] // 2, grid[1]
    pair = {'sh': chip * 2 + 1 - core}
    row = [{'sh': lax.rem(chip + j, n_chip) * 2 + core} for j in range(1, n_chip)]
    col = [{'sw': lax.rem(sw + j, n_sw)} for j in range(1, n_sw)]
    return pair, row, col


DIRECTIONS = [(0, 1), (0, -1), (1, 0), (-1, 0), (1, 1), (1, -1), (-1, 1), (-1, -1)]


def greet(grid, halo, reduce):
    devices = []
    if halo:
        sh, sw = lax.axis_index('sh'), lax.axis_index('sw')
        for dh, dw in DIRECTIONS:
            devices.append({'sh': lax.rem(sh + dh + grid[0], grid[0]), 'sw': lax.rem(sw + dw + grid[1], grid[1])})
    if reduce:
        pair, row, col = peers_of(grid)
        devices += [pair] + row + col
    barrier = pltpu.get_barrier_semaphore()
    for device in devices:
        pl.semaphore_signal(barrier, inc=1, device_id=device, device_id_type=MESH)
    pl.semaphore_wait(barrier, len(devices))


def clear_halo(dm, xp):
    b, r = dm.b, RADIUS
    edge = (dm.nw + 1) * b
    xp[:r] = jnp.zeros((r,) + xp.shape[1:], BF16)
    xp[dm.h + r:] = jnp.zeros((r,) + xp.shape[1:], BF16)
    xp[r:dm.h + r, :b] = jnp.zeros((dm.h, b, dm.cp), BF16)
    xp[r:dm.h + r, edge:] = jnp.zeros((dm.h, b, dm.cp), BF16)


def halo_copies(dm, grid, xp, send_sem, recv_sem):
    sh, sw = lax.axis_index('sh'), lax.axis_index('sw')
    r, b = RADIUS, dm.b
    rows = {1: (dm.h, r, 0), -1: (r, r, dm.h + r), 0: (r, dm.h, r)}
    cols = {1: (dm.nw * b, b, 0), -1: (b, b, (dm.nw + 1) * b), 0: (b, dm.nw * b, b)}

    def inside(a, c):
        return (a >= 0) & (a < grid[0]) & (c >= 0) & (c < grid[1])

    found = []
    for d, (dh, dw) in enumerate(DIRECTIONS):
        r0, rn, rt = rows[dh]
        c0, cn, ct = cols[dw]
        target = {'sh': lax.rem(sh + dh + grid[0], grid[0]), 'sw': lax.rem(sw + dw + grid[1], grid[1])}
        copy = pltpu.make_async_remote_copy(
            src_ref=xp.at[pl.ds(r0, rn), pl.ds(c0, cn)], dst_ref=xp.at[pl.ds(rt, rn), pl.ds(ct, cn)],
            send_sem=send_sem.at[d], recv_sem=recv_sem.at[d], device_id=target, device_id_type=MESH)
        found.append((copy, inside(sh + dh, sw + dw), inside(sh - dh, sw - dw)))
    return found[:2] + found[4:], found[2:4]


def halo_start(copies):
    for copy, sends, _ in copies:
        @pl.when(sends)
        def _():
            copy.start()


def halo_wait(copies):
    for copy, sends, receives in copies:
        @pl.when(sends)
        def _():
            copy.wait_send()

        @pl.when(receives)
        def _():
            copy.wait_recv()


def exchange(slots, mine, devices, send_sem, recv_sem):
    copies = []
    for j, device in enumerate(devices):
        copy = pltpu.make_async_remote_copy(src_ref=slots.at[mine], dst_ref=slots.at[mine], send_sem=send_sem.at[j],
                                            recv_sem=recv_sem.at[j], device_id=device, device_id_type=MESH)
        copies.append(copy)
    return copies


def go(copies):
    for copy in copies:
        copy.start()


def finish(copies):
    for copy in copies:
        copy.wait()


def fold(values, parts):
    return sum(values[:, part] for part in parts)


def sum_slots(slots):
    total = slots[0]
    for j in range(1, slots.shape[0]):
        total = total + slots[j]
    return total


def gather_scratch(grid, block):
    n_chip, n_sw = grid[0] // 2, grid[1]
    dma = pltpu.SemaphoreType.DMA
    return [pltpu.VMEM((n,) + block, F32) for n in (2, n_chip, n_sw)] + [dma((max(n - 1, 1),)) for n in (2, 2, n_chip, n_chip, n_sw, n_sw)]


N_GATHER = 9


def gather_stages(grid, scratch):
    slots, sems = scratch[:3], scratch[3:]
    mine = [position()[1], position()[0], position()[2]]
    pair, row, col = peers_of(grid)
    copies = [exchange(slots[j], mine[j], devices, sems[2 * j], sems[2 * j + 1]) for j, devices in enumerate(([pair], row, col))]

    def stage(j):
        def run():
            if j > 0:
                finish(copies[j - 1])
            if j in (1, 2):
                slots[j][mine[j]] = sum_slots(slots[j - 1])
            if j < 3:
                go(copies[j])
        return run

    return [stage(j) for j in range(4)]


def grn_begin(dm, scratch, sums):
    core = position()[1]
    for j, ref in enumerate(sums):
        scratch[0][core, j] = fold(ref, dm.hs)


def grn_total(dm, grid, sums, scratch):
    grn_begin(dm, scratch, sums)
    for stage in gather_stages(grid, scratch):
        stage()
    return sum_slots(scratch[2])


def spread(dm, ref, values):
    ref[...] = jnp.zeros_like(ref)
    for part in dm.hs:
        ref[:, part] = values


def grn_cross(dm, norm, gamma, cross, dsq_o, ggam_o):
    mean = jnp.mean(norm, axis=-1, keepdims=True) + EPSILON
    d_scale = gamma * cross
    d_norm = d_scale / mean - jnp.sum(d_scale * norm, axis=-1, keepdims=True) / (mean * mean * dm.hid)
    spread(dm, dsq_o, d_norm / norm)
    ggam_o[...] = jnp.sum(cross * (norm / mean), axis=0, keepdims=True)


def grn_coef(dm, norm, gamma, coef_o):
    mean = jnp.mean(norm, axis=-1, keepdims=True) + EPSILON
    spread(dm, coef_o, gamma * (norm / mean) + 1.0)


def prep_kernel(dm, conv_w, conv_b, norm_g, norm_b, fc1_w, fc1_b, beta, fc2_t, fc2_b, mask_i, ones, place, perm, x, dout,
                taps_o, cvec_o, hvec_o, w1_o, w2t_o, gmat_o, mask_o, x_o, d_o):
    for ref in (taps_o, cvec_o, hvec_o, w1_o, w2t_o):
        ref[...] = jnp.zeros_like(ref)
    square = (dm.b, dm.b)
    diagonal = lax.broadcasted_iota(jnp.int32, square, 0) == lax.broadcasted_iota(jnp.int32, square, 1)
    for k in range(2):
        for cs, hs in zip(dm.cs, dm.hs):
            for j, ref in enumerate((conv_b, norm_g, norm_b, fc2_b)):
                cvec_o[k, j:j + 1, cs] = ref[k:k + 1, :]
            for j, ref in enumerate((fc1_b, beta)):
                hvec_o[k, j:j + 1, hs] = ref[k:k + 1, :]
            w1_o[k, cs, hs] = fc1_w[k]
            w2t_o[k, cs, hs] = fc2_t[k]
        column = jnp.sum(jnp.where(diagonal, mask_i[k:k + 1, :], 0.0), axis=1, keepdims=True)
        mask_o[k] = jnp.broadcast_to(column, (dm.b, dm.cp))
    for i in range(TAPS):
        for j in range(TAPS):
            both = conv_w[i, j].astype(F32)
            for k in range(2):
                for cs in dm.cs:
                    taps_o[k, pl.ds(i * 8 + j, 1), cs] = both[k:k + 1]
                    taps_o[2 + k, pl.ds((TAPS - 1 - i) * 8 + TAPS - 1 - j, 1), cs] = both[k:k + 1]
    for k in range(2):
        values = ones[...].astype(F32) * line(cvec_o, k, NORM_G)
        for j in range(3):
            part = values.astype(BF16)
            gmat_o[k, j] = part
            values = values - part.astype(F32)
    moves = move_rows(perm)
    for src, out in ((x, x_o), (dout, d_o)):
        for wg in range(dm.nw):
            joined = sum(dot(src[:, RADIUS * wg + q].reshape(-1, dm.c), place[q]) for q in range(RADIUS)).astype(BF16)
            moved = dot(moves, joined).astype(BF16)
            out[:, wg * dm.b:(wg + 1) * dm.b] = moved.reshape(dm.h, dm.b, dm.cp)


def first_kernel(dm, grid, x, taps, rel, cvec, hvec, ones, w1, gamma,
                 normed_o, inv_o, h_o, phi_o, xp_o, norm_o, coef_o, wide, toep, ss, xp, keep_sem, send, recv, *grn):
    step = pl.program_id(0)

    @pl.when(step == 0)
    def _():
        clear_halo(dm, xp)
        for row in range(dm.h):
            xp[row + RADIUS, dm.inner] = x[row]
        greet(grid, True, True)
        sides, ends = halo_copies(dm, grid, xp, send, recv)
        halo_start(ends)
        halo_start(sides)
        build_toeplitz(dm, taps.at[0], rel, toep)
        ss[...] = jnp.zeros_like(ss)
        halo_wait(ends)
        build_wide(dm, xp, wide, ONE)

    @pl.when(step == dm.half)
    def _():
        halo_wait(halo_copies(dm, grid, xp, send, recv)[0])
        pltpu.make_async_copy(xp, xp_o, keep_sem).start()
        build_wide(dm, xp, wide, TWO)

    forward_tile(dm, ONE, step, wide, toep, cvec, hvec, ones, w1, normed_o, inv_o, h_o)

    def body(rows, lanes):
        g = gelu_chunk(dm, h_o, phi_o, rows, lanes)
        ss[:, lanes] += jnp.sum(per_image(dm, g * g), axis=0)

    lane_loop(dm, body)

    @pl.when(step == pl.num_programs(0) - 1)
    def _():
        pltpu.make_async_copy(xp, xp_o, keep_sem).wait()
        norm = jnp.sqrt(grn_total(dm, grid, [ss], grn)[0])
        norm_o[...] = norm
        grn_coef(dm, norm, gamma[pl.ds(ONE, 1), :], coef_o)


def lead_tile(dm, step):
    return lax.rem(jnp.minimum(step, dm.tiles - 1) + dm.half, dm.tiles)


def halo_schedule(dm, grid, step, xp, wide, send, recv, between, after):
    @pl.when(step == dm.half)
    def _():
        halo_start(halo_copies(dm, grid, xp, send, recv)[0])

    @pl.when(step == dm.tiles)
    def _():
        ends = halo_copies(dm, grid, xp, send, recv)[1]
        halo_start(ends)
        between()
        halo_wait(ends)
        build_wide(dm, xp, wide, ONE)

    @pl.when(step == dm.tiles + dm.half)
    def _():
        halo_wait(halo_copies(dm, grid, xp, send, recv)[0])
        after()
        build_wide(dm, xp, wide, TWO)


def second_kernel(dm, grid, h1, phi1, xp1, coef1, taps, rel, cvec, hvec, ones, w1, w2t, gamma, mask, dout,
                  normed_o, inv_o, h_o, phi_o, dr_o, xp_o, sdr_o, coef_o, dsq_o, ggam_o,
                  wide, toep, resp, raw, ss, cross, tile_s, xp, keep_sem, send, recv, *grn):
    step = pl.program_id(0)
    keep = pltpu.make_async_copy(xp, xp_o, keep_sem)

    @pl.when(step == 0)
    def _():
        clear_halo(dm, xp)
        greet(grid, True, True)
        for ref in (ss, cross, sdr_o):
            ref[...] = jnp.zeros_like(ref)

    halo_schedule(dm, grid, step, xp, wide, send, recv, lambda: build_toeplitz(dm, taps.at[1], rel, toep), keep.start)

    @pl.when(step < dm.tiles)
    def _():
        tile = lead_tile(dm, step)

        def body(rows, lanes):
            g = h1[rows, lanes].astype(F32) * phi1[rows, lanes]
            r = per_image(dm, g) * image_lines(coef1, lanes) + line(hvec, ONE, BETA, lanes)
            resp[rows, lanes] = r.reshape(dm.chunk, 128).astype(BF16)

        lane_loop(dm, body)
        load_tile(dm, xp1, tile_s, tile, dm.b, RADIUS)
        o = (dot_bt(resp[...], w2t[ONE]) + line(cvec, ONE, FC2_B)).reshape(-1, dm.b, dm.cp)
        y = (tile_s[...].astype(F32) + (o * mask[ONE][None]).reshape(-1, dm.cp)).astype(BF16)
        store_tile(dm, xp, y, tile, dm.b, RADIUS)

    @pl.when(step >= dm.tiles)
    def _():
        tile = step - dm.tiles
        forward_tile(dm, TWO, tile, wide, toep, cvec, hvec, ones, w1, normed_o, inv_o, h_o)
        load_tile(dm, dout, tile_s, tile, 0, 0)
        raw[...] = dot(tile_s[...], w2t[TWO])

        def body(rows, lanes):
            g = gelu_chunk(dm, h_o, phi_o, rows, lanes)
            ss[:, lanes] += jnp.sum(per_image(dm, g * g), axis=0)
            cross_chunk(dm, TWO, raw, mask, g, dr_o, cross, sdr_o, rows, lanes)

        lane_loop(dm, body)

    @pl.when(step == pl.num_programs(0) - 1)
    def _():
        keep.wait()
        total = grn_total(dm, grid, [ss, cross], grn)
        norm = jnp.sqrt(total[0])
        grn_coef(dm, norm, gamma[pl.ds(TWO, 1), :], coef_o)
        grn_cross(dm, norm, gamma[pl.ds(TWO, 1), :], total[1], dsq_o, ggam_o)


def backward_tile(dm, k, h_i, phi_i, dr_i, coef, dsq, dout, normed_i, inv_i, cvec, hvec, ones, gmat, w1, w2t, mask,
                  resp, dh, gfc1, gfc2, sdh, sums, x_rows):
    def body(rows, lanes):
        hv = h_i[rows, lanes].astype(F32)
        phi = phi_i[rows, lanes]
        g = per_image(dm, hv * phi)
        a = image_lines(coef, lanes)
        resp[rows, lanes] = (g * a + line(hvec, k, BETA, lanes)).reshape(dm.chunk, 128).astype(BF16)
        slope = phi + hv * (np.float32(0.3989422804014327) * jnp.exp(-0.5 * hv * hv))
        dg = per_image(dm, dr_i[rows, lanes].astype(F32)) * a + g * image_lines(dsq, lanes)
        dhv = (dg.reshape(dm.chunk, 128) * slope).astype(BF16)
        dh[rows, lanes] = dhv
        sdh[:, lanes] += jnp.sum(per_image(dm, dhv.astype(F32)), axis=0)

    lane_loop(dm, body)
    dsel32 = jnp.where((mask[k] != 0.0)[None], dout[...].astype(F32).reshape(-1, dm.b, dm.cp), 0.0)
    sums[FC2_B] += jnp.sum(dsel32, axis=0)
    gfc2[...] += dot_t(dsel32.reshape(-1, dm.cp).astype(BF16), resp[...])
    y = None
    if x_rows is not None:
        o = (dot_bt(resp[...], w2t[k]) + line(cvec, k, FC2_B)).reshape(-1, dm.b, dm.cp)
        y = (x_rows[...].astype(F32) + (o * mask[k][None]).reshape(-1, dm.cp)).astype(BF16)
    normed = normed_i[...]
    norm_g = line(cvec, k, NORM_G)
    n = (normed * norm_g + line(cvec, k, NORM_B)).astype(BF16)
    gfc1[...] += dot_t(n, dh[...])
    dn16 = dot_bt(dh[...], w1[k]).astype(BF16)
    dn = dn16.astype(F32)
    scale = np.float32(1.0 / dm.c)
    mean1 = (dot_bt(dn16, gmat[k, 0]) + dot_bt(dn16, gmat[k, 1]) + dot_bt(dn16, gmat[k, 2])) * scale
    dnormed = dn * norm_g
    mean2 = dot_split(dnormed * normed, ones[...]) * scale
    dconv = (inv_i[...] * (dnormed - mean1 - normed * mean2)).astype(BF16)

    for row, values in ((CONV_B, dconv.astype(F32)), (NORM_G, dn * normed), (NORM_B, dn)):
        sums[row] += jnp.sum(values.reshape(-1, dm.b, dm.cp), axis=0)
    return dconv, y


def wgrad(dm, wide, dcol, rel, out, stages):
    keep = rel[...] > -50

    def body(i, carry):
        res = None
        for pair in range(2):
            rows = pl.ds(pl.multiple_of(pair * dm.tall + i * dm.rw, 16), dm.block)
            part = dot(dcol[:, pair * dm.block:(pair + 1) * dm.block], wide[rows, :])
            res = part if res is None else res + part
        for g in range(RADIUS):
            part = jnp.where(keep, res[:, dm.lanes(g)], 0.0)
            for q in range(RADIUS):
                out[q, pl.ds(i, 1), dm.lanes(g)] = jnp.sum(part[dm.cs[q]], axis=0, keepdims=True)
        for tap, stage in stages.items():
            pl.when(i == tap)(stage)
        return carry

    loop(TAPS, body)


def vector_rows(dm):
    return 2 * dm.c


def conv_rows(dm):
    return round_up(2 * dm.c + 6, 8)


def pack_conv(dm, out, base, corr):
    for j in range(TAPS):
        total = None
        for q in range(RADIUS):
            lane = ((q + j) // RADIUS) * dm.cp + ((q + j) % RADIUS) * dm.c
            part = corr[q, :, lane:lane + dm.c]
            total = part if total is None else total + part
        out[base + 8 * j:base + 8 * j + 8, :dm.c] = total


def pack_grads(dm, pack, gfc1, gfc2, sdh, sdr, sums):
    for base, ref in ((0, gfc1), (dm.c, gfc2)):
        pack[base:base + dm.c, :dm.hid] = sum(ref[cs, hs] for cs, hs in zip(dm.cs, dm.hs))
    base = vector_rows(dm)
    rows = [fold(jnp.sum(ref[...], axis=0, keepdims=True), dm.hs) for ref in (sdh, sdr)]
    rows += [fold(jnp.sum(sums[row], axis=0, keepdims=True), dm.cs) for row in range(4)]
    for j, row in enumerate(rows):
        pack[base + j:base + j + 1, :row.shape[1]] = row


def pack_shape(dm, grid, conv):
    rows = conv_rows(dm) + (8 * TAPS if conv else 0)
    return (round_up(rows, 8 * grid[0]), round_up(dm.hid, 128))


def conv_shape(dm):
    return (8 * TAPS, 128)


def sum_scratch(grid, shape):
    rows, lanes = shape
    n_chip, n_sw = grid[0] // 2, grid[1]
    dma = pltpu.SemaphoreType.DMA
    return ([pltpu.VMEM((rows // 2, lanes), F32)]
            + [pltpu.VMEM((n, rows // (2 * n_chip), lanes), F32) for n in (n_chip, n_chip, n_chip, n_sw)]
            + [dma((n,)) for n in (1, 1, n_chip - 1, n_chip - 1, n_sw - 1, n_sw - 1, n_chip - 1, n_chip - 1, 1, 1)])


N_SUM = 15


def sum_stages(grid, x, out, scratch):
    got1, half, got2, part, slots3, send1, recv1, send2, recv2, send3, recv3, send4, recv4, send5, recv5 = scratch
    chip, core, sw = position()
    n_chip = grid[0] // 2
    pair, row, col = peers_of(grid)
    rows = got1.shape[0]
    chunk = half.shape[1]

    def whole(ref, which):
        return ref.at[pl.ds(pl.multiple_of(which * rows, 8), rows)]

    def copies1():
        return [pltpu.make_async_remote_copy(src_ref=whole(x, 1 - core), dst_ref=got1, send_sem=send1.at[0], recv_sem=recv1.at[0],
                                             device_id=pair, device_id_type=MESH)]

    def copies2():
        made = []
        for j, device in enumerate(row):
            made.append(pltpu.make_async_remote_copy(
                src_ref=half.at[lax.rem(chip + j + 1, n_chip)], dst_ref=got2.at[chip], send_sem=send2.at[j],
                recv_sem=recv2.at[j], device_id=device, device_id_type=MESH))
        return made

    def copies5():
        return [pltpu.make_async_remote_copy(src_ref=whole(out, core), dst_ref=whole(out, core), send_sem=send5.at[0],
                                             recv_sem=recv5.at[0], device_id=pair, device_id_type=MESH)]

    def stage0():
        go(copies1())

    def stage1():
        finish(copies1())
        for j in range(n_chip):
            start = pl.multiple_of(core * rows + j * chunk, 8)
            half[j] = x[pl.ds(start, chunk)] + got1[j * chunk:(j + 1) * chunk]
        go(copies2())

    def stage2():
        got2[chip] = half[chip]
        finish(copies2())
        slots3[sw] = sum_slots(got2)
        go(exchange(slots3, sw, col, send3, recv3))

    def stage3():
        finish(exchange(slots3, sw, col, send3, recv3))
        part[chip] = sum_slots(slots3)
        go(exchange(part, chip, row, send4, recv4))

    def stage4():
        finish(exchange(part, chip, row, send4, recv4))
        for j in range(n_chip):
            out[pl.ds(pl.multiple_of(core * rows + j * chunk, 8), chunk)] = part[j]
        go(copies5())

    def stage5():
        finish(copies5())

    return [stage0, stage1, stage2, stage3, stage4, stage5]


def backward_phase(dm, step, k, dp, dcol, args, x_rows):
    tile = lead_tile(dm, step)
    dconv, y = backward_tile(dm, k, *args, x_rows)
    store_tile(dm, dp, dconv, tile, dm.b, RADIUS)
    dcol[:, pl.ds(pl.multiple_of(tile * dm.m, 128), dm.m)] = dconv.T
    return tile, y


def third_kernel(dm, grid, h2, phi2, dr2, coef2, dsq2, dout, normed, inv, xp2, h1, phi1, norm1, taps, rel, cvec, hvec, ones, gmat,
                 w1, w2t, gamma, mask, sdr2,
                 y_o, d1_o, dr1_o, pack, sdr_o, dsq_o, ggam_o,
                 wide, toep, dp, dcol, corr, resp, dh, tile_s, gfc1, gfc2, sdh, sums, raw, tile_x, cross, send, recv, *grn):
    step = pl.program_id(0)

    @pl.when(step == 0)
    def _():
        clear_halo(dm, dp)
        greet(grid, True, True)
        for ref in (cross, sdr_o, gfc1, gfc2, sdh, sums, corr, pack):
            ref[...] = jnp.zeros_like(ref)

    halo_schedule(dm, grid, step, dp, wide, send, recv, lambda: build_toeplitz(dm, taps.at[3], rel, toep), lambda: None)

    @pl.when(step < dm.tiles)
    def _():
        load_tile(dm, dout, tile_s, lead_tile(dm, step), 0, 0)
        load_tile(dm, xp2, tile_x, lead_tile(dm, step), dm.b, RADIUS)
        tile, y = backward_phase(dm, step, TWO, dp, dcol, (h2, phi2, dr2, coef2, dsq2, tile_s, normed, inv, cvec, hvec, ones, gmat,
                                                           w1, w2t, mask, resp, dh, gfc1, gfc2, sdh, sums), tile_x)
        store_tile(dm, y_o, y, tile, 0, 0)

    @pl.when(step >= dm.tiles)
    def _():
        tile = step - dm.tiles
        load_tile(dm, dout, tile_s, tile, 0, 0)
        din = (tile_s[...].astype(F32) + conv_tile(dm, wide, toep, tile)).astype(BF16)
        d1_o[...] = din
        raw[...] = dot(din, w2t[ONE])

        def body(rows, lanes):
            g = h1[rows, lanes].astype(F32) * phi1[rows, lanes]
            cross_chunk(dm, ONE, raw, mask, g, dr1_o, cross, sdr_o, rows, lanes)

        lane_loop(dm, body)

    @pl.when(step == pl.num_programs(0) - 1)
    def _():
        begin, row, col, end = gather_stages(grid, grn)
        grn_begin(dm, grn, [cross])
        begin()
        build_wide(dm, xp2, wide, ONE)
        build_wide(dm, xp2, wide, TWO)
        pack_grads(dm, pack, gfc1, gfc2, sdh, sdr2, sums)
        wgrad(dm, wide, dcol, rel, corr, {ONE: row, RADIUS: col})
        pack_conv(dm, pack, conv_rows(dm), corr)
        end()
        grn_cross(dm, norm1[...], gamma[pl.ds(ONE, 1), :], sum_slots(grn[2])[0], dsq_o, ggam_o)


def fourth_kernel(dm, grid, h1, phi1, dr1, coef1, dsq1, d1, normed, inv, xp1, taps, rel, cvec, hvec, ones, gmat,
                  w1, w2t, mask, sdr1, pack2_i,
                  d0_o, out1_o, out2_o, conv_o,
                  wide, toep, dp, dcol, corr, resp, dh, tile_s, gfc1, gfc2, sdh, sums, pack1, out1, pack2, out2, send, recv, *sem):
    step = pl.program_id(0)
    stages1 = sum_stages(grid, pack1, out1, sem[:N_SUM])
    stages2 = sum_stages(grid, pack2, out2, sem[N_SUM:2 * N_SUM])
    conv_sem = sem[2 * N_SUM:]
    conv_stages = gather_stages(grid, conv_sem)

    @pl.when(step == 0)
    def _():
        clear_halo(dm, dp)
        greet(grid, True, True)
        for ref in (gfc1, gfc2, sdh, sums, corr, pack1):
            ref[...] = jnp.zeros_like(ref)
        pack2[...] = pack2_i[...]

    begin1, *middle1, end1 = stages1
    conv_begin, conv_row, conv_col, conv_end = conv_stages
    a, b, c, d, e, f = stages2
    plan = [[a], [b], [], [c], [d], [e], [], [f, conv_row], [], [middle1.pop()], [conv_col]]
    for at, jobs in enumerate(plan):
        @pl.when(step == at)
        def _():
            for job in jobs:
                job()

    def between():
        pack_grads(dm, pack1, gfc1, gfc2, sdh, sdr1, sums)
        begin1()
        build_toeplitz(dm, taps.at[2], rel, toep)
        build_wide(dm, xp1, wide, ONE)
        build_wide(dm, xp1, wide, TWO)
        half, chip, column = middle1
        half()
        wgrad(dm, wide, dcol, rel, corr, {RADIUS: chip})
        core = position()[1]
        conv_sem[0][core] = jnp.zeros(conv_shape(dm), F32)
        pack_conv(dm, conv_sem[0].at[core], 0, corr)
        conv_begin()
        column()

    halo_schedule(dm, grid, step, dp, wide, send, recv, between, lambda: None)

    @pl.when(step < dm.tiles)
    def _():
        backward_phase(dm, step, ONE, dp, dcol, (h1, phi1, dr1, coef1, dsq1, d1, normed, inv, cvec, hvec, ones, gmat,
                                                 w1, w2t, mask, resp, dh, gfc1, gfc2, sdh, sums), None)

    @pl.when(step >= dm.tiles)
    def _():
        tile = step - dm.tiles
        din = (d1[...].astype(F32) + conv_tile(dm, wide, toep, tile)).astype(BF16)
        store_tile(dm, d0_o, din, tile, 0, 0)

    @pl.when(step == pl.num_programs(0) - 1)
    def _():
        end1()
        out1_o[...] = out1[...]
        out2_o[...] = out2[...]
        conv_end()
        conv_o[...] = sum_slots(conv_sem[2])


def final_kernel(dm, out1, out2, conv1, ggam1, ggam2, y, d, place, perm, yo, do, gcw, gcb, gng, gnb, gf1w, gf1b, ggam, gbeta, gf2w, gf2b):
    c, hid = dm.c, dm.hid
    ggam[...] = jnp.concatenate([ggam1[...], ggam2[...]], axis=0)
    for k, ref in enumerate((out1, out2)):
        gf1w[k] = ref[:c, :hid]
        gf2w[k] = ref[c:2 * c, :hid] * np.float32(KEEP)
        base = vector_rows(dm)
        for row, out in enumerate((gf1b, gbeta, gcb, gng, gnb, gf2b)):
            value = ref[base + row:base + row + 1, :out.shape[1]]
            out[k:k + 1, :] = value * np.float32(KEEP) if out is gf2b else value
    for k, (ref, base) in enumerate(((conv1, 0), (out2, conv_rows(dm)))):
        for j in range(TAPS):
            for i in range(TAPS):
                row = base + 8 * j + i
                gcw[i, j, k:k + 1, :] = ref[row:row + 1, :c]
    moves = move_rows(perm)
    for src, out in ((y, yo), (d, do)):
        for wg in range(dm.nw):
            rows = src[:, wg * dm.b:(wg + 1) * dm.b].reshape(-1, dm.cp)
            moved = dot(moves, rows).astype(BF16)
            for q in range(RADIUS):
                out[:, RADIUS * wg + q] = dot_bt(moved, place[q]).astype(BF16).reshape(dm.b, dm.h, dm.c)


def constants(dm):
    index = np.arange(dm.cp)
    col, chan = index // dm.c, index % dm.c
    live = (index[:, None] < RADIUS * dm.c) & (index[None, :] < RADIUS * dm.c)
    rel = np.where((chan[:, None] == chan[None, :]) & live, col[:, None] - col[None, :], -100).astype(np.int32)
    ones = ((col[:, None] == col[None, :]) & live).astype(np.float32)
    place = np.stack([np.eye(dm.c, dm.cp, q * dm.c) for q in range(RADIUS)])
    count = dm.h * dm.b
    order = np.arange(count, dtype=np.int32)
    moves = [order.reshape(shape).T.reshape(1, count) for shape in ((dm.h, dm.b), (dm.b, dm.h))]
    return [jnp.asarray(a) for a in [rel] + moves] + [jnp.asarray(a, BF16) for a in (ones, place)]


def move_rows(ref):
    count = ref.shape[1]
    rows = lax.broadcasted_iota(jnp.int32, (count, count), 0)
    return jnp.where(rows == ref[...], 1.0, 0.0).astype(BF16)


def call(dm, kernel, steps, ins, outs, scratch, name, cid):
    def spec(shape, mode):
        if mode is WHOLE:
            return FULL
        if mode == 'any':
            return pl.BlockSpec(memory_space=pl.ANY)
        maps = {'lead': lambda s: (lead_tile(dm, s), 0),
                'tail': lambda s: (jnp.maximum(s - dm.tiles, 0), 0),
                'both': lambda s: (jnp.where(s < dm.tiles, lead_tile(dm, s), s - dm.tiles), 0),
                'only': lambda s: (s, 0)}
        return pl.BlockSpec((dm.m, shape[1]), maps[mode])

    return pl.pallas_call(
        kernel, grid=(steps,), in_specs=[spec(a.shape, mode) for a, mode in ins],
        out_specs=[spec(shape, mode) for shape, _, mode in outs],
        out_shape=[jax.ShapeDtypeStruct(shape, dtype) for shape, dtype, _ in outs],
        scratch_shapes=scratch, name=name,
        compiler_params=pltpu.CompilerParams(dimension_semantics=('arbitrary',), vmem_limit_bytes=VMEM_LIMIT,
                                             collective_id=cid, has_side_effects=True))(*[a for a, _ in ins])


def solution(mesh):
    grid = (mesh.shape['sh'], mesh.shape['sw'])
    act_spec = P('dp', 'sh', 'sw', WHOLE)
    replicated = P()

    def local_step(act_in, drop_mask, grad_out, conv_w, conv_b, norm_g, norm_b, fc1_w, fc1_b, gamma, grn_beta, fc2_w, fc2_b):
        dm = Dims(act_in.shape, fc1_w.shape[-1])
        rel, perm, perm_back, ones, place = constants(dm)
        sds = jax.ShapeDtypeStruct
        c_shape, h_shape, s_shape, n_shape = (dm.rows, dm.cp), (dm.rows, dm.hp), (dm.b, dm.hp), (dm.b, dm.hid)
        x_shape = (dm.h, dm.nw * dm.b, dm.cp)
        act_t = (dm.b, dm.w, dm.h, dm.c)
        swap = (0, 2, 1, 3)
        big = pltpu.CompilerParams(vmem_limit_bytes=VMEM_LIMIT)
        taps, cvec, hvec, w1, w2t, gmat, mask, x1, d2 = pl.pallas_call(
            functools.partial(prep_kernel, dm),
            out_shape=[sds((4, TAPS * 8, dm.cp), F32), sds((2, 4, dm.cp), F32), sds((2, 2, dm.hp), F32), sds((2, dm.cp, dm.hp), BF16),
                       sds((2, dm.cp, dm.hp), BF16), sds((2, 3, dm.cp, dm.cp), BF16), sds((2, dm.b, dm.cp), F32),
                       sds(x_shape, BF16), sds(x_shape, BF16)],
            in_specs=[FULL] * 15, out_specs=[FULL] * 9, compiler_params=big, name='prep')(
                conv_w.transpose(1, 2, 0, 3), conv_b, norm_g, norm_b, fc1_w, fc1_b, grn_beta, fc2_w.transpose(0, 2, 1), fc2_b,
                drop_mask.T, ones, place, perm, act_in.transpose(swap), grad_out.transpose(swap))

        dma = pltpu.SemaphoreType.DMA
        V = pltpu.VMEM
        wide_s = V((2 * dm.tall, 3 * dm.cp), BF16)
        toep_s = V((TAPS * 3 * dm.cp, dm.cp), BF16)
        raw_s, hid_s, tile_s = V((dm.m, dm.hp), F32), V((dm.m, dm.hp), BF16), V((dm.m, dm.cp), BF16)
        img_s, acc_s = V(s_shape, F32), V((dm.cp, dm.hp), F32)
        xp_shape = (dm.h + 2 * RADIUS, (dm.nw + 2) * dm.b, dm.cp)
        xp_s = V(xp_shape, BF16)
        halo_s = [dma((8,)), dma((8,))]
        g_shape = (1, dm.hid)
        p1_shape, p2_shape = (pack_shape(dm, grid, conv) for conv in (False, True))

        def wholes(*arrays):
            return [(a, WHOLE) for a in arrays]

        def grn_s(count):
            return gather_scratch(grid, (count, dm.b, dm.hid))

        normed1, inv1, h1, phi1, xp1, norm1, coef1 = call(
            dm, functools.partial(first_kernel, dm, grid), dm.tiles, wholes(x1, taps, rel, cvec, hvec, ones, w1, gamma),
            [(c_shape, F32, 'only'), (c_shape, F32, 'only'), (h_shape, BF16, 'only'), (h_shape, F32, 'only'), (xp_shape, BF16, 'any'),
             (n_shape, F32, WHOLE), (s_shape, F32, WHOLE)],
            [wide_s, toep_s, img_s, xp_s, dma] + halo_s + grn_s(1), 'first', 0)

        normed2, inv2, h2, phi2, dr2, xp2, sdr2, coef2, dsq2, ggam2 = call(
            dm, functools.partial(second_kernel, dm, grid), 2 * dm.tiles,
            [(h1, 'lead'), (phi1, 'lead')] + wholes(xp1, coef1, taps, rel, cvec, hvec, ones, w1, w2t, gamma, mask, d2),
            [(c_shape, F32, 'tail'), (c_shape, F32, 'tail'), (h_shape, BF16, 'tail'), (h_shape, F32, 'tail'), (h_shape, BF16, 'tail'),
             (xp_shape, BF16, 'any')] + [(s_shape, F32, WHOLE)] * 3 + [(g_shape, F32, WHOLE)],
            [wide_s, toep_s, hid_s, raw_s, img_s, img_s, tile_s, xp_s, dma] + halo_s + grn_s(2), 'second', 1)

        bwd_s = [wide_s, toep_s, xp_s, V((dm.cp, dm.rows), BF16), V((3, 8, 3 * dm.cp), F32), hid_s, hid_s, tile_s,
                 acc_s, acc_s, img_s, V((4, dm.b, dm.cp), F32)]
        y2, d1, dr1, pack2, sdr1, dsq1, ggam1 = call(
            dm, functools.partial(third_kernel, dm, grid), 2 * dm.tiles,
            [(h2, 'lead'), (phi2, 'lead'), (dr2, 'lead')] + wholes(coef2, dsq2, d2) + [(normed2, 'lead'), (inv2, 'lead')] + wholes(xp2)
            + [(h1, 'tail'), (phi1, 'tail')] + wholes(norm1, taps, rel, cvec, hvec, ones, gmat, w1, w2t, gamma, mask, sdr2),
            [(x_shape, BF16, WHOLE), (c_shape, BF16, 'tail'), (h_shape, BF16, 'tail'), (p2_shape, F32, WHOLE), (s_shape, F32, WHOLE),
             (s_shape, F32, WHOLE), (g_shape, F32, WHOLE)],
            bwd_s + [raw_s, tile_s, img_s] + halo_s + grn_s(1), 'third', 2)

        d0, out1, out2, conv1 = call(
            dm, functools.partial(fourth_kernel, dm, grid), 2 * dm.tiles,
            [(h1, 'lead'), (phi1, 'lead'), (dr1, 'lead')] + wholes(coef1, dsq1) + [(d1, 'both'), (normed1, 'lead'), (inv1, 'lead')]
            + wholes(xp1, taps, rel, cvec, hvec, ones, gmat, w1, w2t, mask, sdr1, pack2),
            [(x_shape, BF16, WHOLE), (p1_shape, F32, WHOLE), (p2_shape, F32, WHOLE), (conv_shape(dm), F32, WHOLE)],
            bwd_s + [V(p1_shape, F32)] * 2 + [V(p2_shape, F32)] * 2 + halo_s + sum_scratch(grid, p1_shape) + sum_scratch(grid, p2_shape)
            + gather_scratch(grid, conv_shape(dm)), 'fourth', 3)

        conv_t, fc2_t = (TAPS, TAPS, 2, dm.c), (2, dm.c, dm.hid)
        y_t, d_t, gcw, gcb, gng, gnb, gf1w, gf1b, ggam, gbeta, gf2w, gf2b = pl.pallas_call(
            functools.partial(final_kernel, dm),
            out_shape=[sds(act_t, BF16)] * 2 + [sds(shape, F32) for shape in (
                conv_t, conv_b.shape, norm_g.shape, norm_b.shape, fc1_w.shape, fc1_b.shape, gamma.shape, grn_beta.shape, fc2_t, fc2_b.shape)],
            in_specs=[FULL] * 9, out_specs=[FULL] * 12, compiler_params=big, name='final')(
                out1, out2, conv1, ggam1, ggam2, y2, d0, place, perm_back)
        return (y_t.transpose(swap), d_t.transpose(swap), gcw.transpose(2, 0, 1, 3), gcb, gng, gnb, gf1w, gf1b, ggam, gbeta,
                gf2w.transpose(0, 2, 1), gf2b)

    return jax.shard_map(local_step, mesh=mesh,
                         in_specs=(act_spec, P('dp', WHOLE), act_spec) + (replicated,) * 10,
                         out_specs=(act_spec, act_spec) + (P('dp'),) * 10,
                         check_vma=False)
```

```python
import functools

import jax
import jax.numpy as jnp
import numpy as np
from jax import lax
from jax.experimental import pallas as pl
from jax.experimental.pallas import tpu as pltpu
from jax.sharding import PartitionSpec as P

EPSILON = 1e-6
RADIUS = 3
TAPS = 2 * RADIUS + 1
CHUNKS = 1
MESH = pl.DeviceIdType.MESH
F32 = jnp.float32
BF16 = jnp.bfloat16
KEEP = 4.0 / 3.0
VMEM_LIMIT = 60 * 1024 * 1024
FULL = pl.BlockSpec(memory_space=pltpu.VMEM)
WHOLE = None
CONV_B, NORM_G, NORM_B, FC2_B = range(4)
FC1_B, BETA = range(2)
ONE, TWO = range(2)


def round_up(value, unit):
    return (value + unit - 1) // unit * unit


class Dims:
    def lanes(self, g):
        return slice(g * self.cp, (g + 1) * self.cp)

    def __init__(self, act_shape, hidden):
        self.b, self.h, self.w, self.c = act_shape
        self.hid = hidden
        self.nw = self.w // RADIUS
        self.cp = round_up(RADIUS * self.c, 128)
        self.hp = round_up(RADIUS * hidden, 128)
        self.pairs = ((1, 2), (0, self.nw - 1))
        self.rw = 2 * self.b
        self.pitch = self.hp + 128
        self.chunk = 2 * self.rw
        self.th = self.h // RADIUS
        self.half = RADIUS
        self.tiles = 2 * self.half
        self.m = self.th * self.rw
        self.rows = self.h * self.nw * self.b
        self.block = self.h * self.rw
        self.tall = (self.h + 2 * RADIUS) * self.rw
        self.inner = slice(self.b, self.b + self.nw * self.b)
        self.cs = [slice(q * self.c, (q + 1) * self.c) for q in range(RADIUS)]
        self.hs = [slice(q * hidden, (q + 1) * hidden) for q in range(RADIUS)]


def loop(count, body, init=0):
    return lax.fori_loop(0, count, body, init)


def dot(lhs, rhs):
    return jnp.dot(lhs, rhs, preferred_element_type=F32)


def dot_t(lhs, rhs):
    return lax.dot_general(lhs, rhs, (((0,), (0,)), ((), ())), preferred_element_type=F32)


def dot_split(values, rhs):
    hi = values.astype(BF16)
    rest = values - hi.astype(F32)
    mid = rest.astype(BF16)
    low = (rest - mid.astype(F32)).astype(BF16)
    return dot(hi, rhs) + dot(mid, rhs) + dot(low, rhs)


def build_wide(dm, src_ref, wide, pair):
    def body(row, carry):
        rows = pl.ds(pl.multiple_of(pair * dm.tall + row * dm.rw, 16), dm.rw)
        for g in range(RADIUS):
            parts = [src_ref[row, (wg + g) * dm.b:(wg + g + 1) * dm.b] for wg in dm.pairs[pair]]
            wide[rows, dm.lanes(g)] = jnp.concatenate(parts, axis=0)
        return carry

    loop(dm.h + 2 * RADIUS, body)


def each_part(dm, tile, col0, body):
    row0 = lax.rem(tile, dm.half) * dm.th
    for pair, groups in enumerate(dm.pairs):
        @pl.when(tile // dm.half == pair)
        def _():
            for r in range(dm.th):
                for j, wg in enumerate(groups):
                    at, col = r * dm.rw + j * dm.b, col0 + wg * dm.b
                    body(slice(at, at + dm.b), row0 + r, slice(col, col + dm.b))


def load_tile(dm, ref, tile_ref, tile, col0, row_off):
    def body(part, row, cols):
        tile_ref[part] = ref[row + row_off, cols]

    each_part(dm, tile, col0, body)


def store_tile(dm, ref, values, tile, col0, row_off):
    def body(part, row, cols):
        ref[row + row_off, cols] = values[part]

    each_part(dm, tile, col0, body)


def build_toeplitz(dm, taps_ref, rel_ref, toep):
    def body(i, carry):
        for g in range(RADIUS):
            acc = jnp.zeros((dm.cp, dm.cp), F32)
            for dj in range(-2, 3):
                j = 3 * g + dj
                if 0 <= j < TAPS:
                    acc = jnp.where(rel_ref[...] == dj, taps_ref[pl.ds(i * 8 + j, 1), :], acc)
            toep[pl.ds(pl.multiple_of((i * 3 + g) * dm.cp, 16), dm.cp), :] = acc.astype(BF16)
        return carry

    loop(TAPS, body)


def conv_pair(dm, wide, toep, tile, acc_s):
    size = dm.block // CHUNKS

    @pl.when(lax.rem(tile, dm.half) == 0)
    def _():
        base = (tile // dm.half) * dm.tall

        def body(c, carry):
            acc = None
            for i in range(TAPS):
                rows = pl.ds(pl.multiple_of(base + c * size + i * dm.rw, 16), size)
                part = dot(wide[rows, :], toep[i * 3 * dm.cp:(i + 1) * 3 * dm.cp, :])
                acc = part if acc is None else acc + part
            acc_s[pl.ds(pl.multiple_of(c * size, 16), size), :] = acc
            return carry

        loop(CHUNKS, body)


def conv_tile(dm, wide, toep, tile, acc_s):
    conv_pair(dm, wide, toep, tile, acc_s)
    return acc_s[pl.ds(pl.multiple_of(lax.rem(tile, dm.half) * dm.m, 16), dm.m), :]


def lane_loop(dm, body):
    def outer(r, carry):
        def inner(lane, c2):
            body(pl.ds(pl.multiple_of(r * dm.chunk, 16), dm.chunk), pl.ds(pl.multiple_of(lane * 128, 128), 128))
            return c2
        return loop(dm.hp // 128, inner, carry)
    loop(dm.m // dm.chunk, outer)


def line(ref, k, row, lanes=slice(None)):
    return ref[k, row:row + 1, lanes]


def image_lines(ref, lanes):
    return ref[:, lanes][None]


def per_image(dm, values):
    return values.reshape(-1, dm.b, values.shape[-1])


def phi_of(hv):
    return 0.5 + 0.5 * lax.erf(hv * np.float32(0.7071067811865476))


def gelu_chunk(dm, h_ref, phi_ref, rows, lanes):
    hv = h_ref[rows, lanes].astype(F32)
    phi = phi_of(hv)
    phi_ref[rows, lanes] = phi
    return hv * phi


def forward_tile(dm, k, tile, wide, toep, acc_s, cvec, hvec, ones, w1, normed_o, inv_o, h_o):
    d = (conv_tile(dm, wide, toep, tile, acc_s) + line(cvec, k, CONV_B)).astype(BF16)
    mean = dot(d, ones[...]) * np.float32(1.0 / dm.c)
    centered = d.astype(F32) - mean
    var = dot_split(centered * centered, ones[...]) * np.float32(1.0 / dm.c)
    inv = lax.rsqrt(var + EPSILON)
    normed = centered * inv
    normed_o[...] = normed
    inv_o[...] = inv
    n = (normed * line(cvec, k, NORM_G) + line(cvec, k, NORM_B)).astype(BF16)
    h_o[:, :dm.hp] = (dot(n, w1[k, :, :dm.hp]) + line(hvec, k, FC1_B)).astype(BF16)


def dot_bt(lhs, rhs):
    return lax.dot_general(lhs, rhs, (((1,), (1,)), ((), ())), preferred_element_type=F32)


def cross_chunk(dm, k, raw, mask, g, dr_o, cross, sdr, rows, lanes):
    dr = (per_image(dm, raw[rows, lanes]) * mask[k, :, :128][None]).astype(BF16)
    dr_o[rows, lanes] = dr.reshape(dm.chunk, 128)
    dr32 = dr.astype(F32)
    cross[:, lanes] += jnp.sum(dr32 * per_image(dm, g), axis=0)
    sdr[:, lanes] += jnp.sum(dr32, axis=0)


def position():
    sh = lax.axis_index('sh')
    return sh // 2, sh % 2, lax.axis_index('sw')


def peers_of(grid):
    chip, core, sw = position()
    n_chip, n_sw = grid[0] // 2, grid[1]
    pair = {'sh': chip * 2 + 1 - core}
    row = [{'sh': lax.rem(chip + j, n_chip) * 2 + core} for j in range(1, n_chip)]
    col = [{'sw': lax.rem(sw + j, n_sw)} for j in range(1, n_sw)]
    return pair, row, col


DIRECTIONS = [(0, 1), (0, -1), (1, 0), (-1, 0), (1, 1), (1, -1), (-1, 1), (-1, -1)]


def greet(grid, halo, reduce):
    devices = []
    if halo:
        sh, sw = lax.axis_index('sh'), lax.axis_index('sw')
        for dh, dw in DIRECTIONS:
            devices.append({'sh': lax.rem(sh + dh + grid[0], grid[0]), 'sw': lax.rem(sw + dw + grid[1], grid[1])})
    if reduce:
        pair, row, col = peers_of(grid)
        devices += [pair] + row + col
    barrier = pltpu.get_barrier_semaphore()
    for device in devices:
        pl.semaphore_signal(barrier, inc=1, device_id=device, device_id_type=MESH)
    pl.semaphore_wait(barrier, len(devices))


def clear_halo(dm, xp):
    b, r = dm.b, RADIUS
    edge = (dm.nw + 1) * b
    xp[:r] = jnp.zeros((r,) + xp.shape[1:], BF16)
    xp[dm.h + r:] = jnp.zeros((r,) + xp.shape[1:], BF16)
    xp[r:dm.h + r, :b] = jnp.zeros((dm.h, b, dm.cp), BF16)
    xp[r:dm.h + r, edge:] = jnp.zeros((dm.h, b, dm.cp), BF16)


def halo_copies(dm, grid, xp, send_sem, recv_sem):
    sh, sw = lax.axis_index('sh'), lax.axis_index('sw')
    r, b = RADIUS, dm.b
    rows = {1: (dm.h, r, 0), -1: (r, r, dm.h + r), 0: (r, dm.h, r)}
    cols = {1: (dm.nw * b, b, 0), -1: (b, b, (dm.nw + 1) * b), 0: (b, dm.nw * b, b)}

    def inside(a, c):
        return (a >= 0) & (a < grid[0]) & (c >= 0) & (c < grid[1])

    found = []
    for d, (dh, dw) in enumerate(DIRECTIONS):
        r0, rn, rt = rows[dh]
        c0, cn, ct = cols[dw]
        target = {'sh': lax.rem(sh + dh + grid[0], grid[0]), 'sw': lax.rem(sw + dw + grid[1], grid[1])}
        copy = pltpu.make_async_remote_copy(
            src_ref=xp.at[pl.ds(r0, rn), pl.ds(c0, cn)], dst_ref=xp.at[pl.ds(rt, rn), pl.ds(ct, cn)],
            send_sem=send_sem.at[d], recv_sem=recv_sem.at[d], device_id=target, device_id_type=MESH)
        found.append((copy, inside(sh + dh, sw + dw), inside(sh - dh, sw - dw)))
    return found[:2] + found[4:], found[2:4]


def halo_start(copies):
    for copy, sends, _ in copies:
        @pl.when(sends)
        def _():
            copy.start()


def halo_wait(copies):
    for copy, sends, receives in copies:
        @pl.when(sends)
        def _():
            copy.wait_send()

        @pl.when(receives)
        def _():
            copy.wait_recv()


def exchange(slots, mine, devices, send_sem, recv_sem):
    copies = []
    for j, device in enumerate(devices):
        copy = pltpu.make_async_remote_copy(src_ref=slots.at[mine], dst_ref=slots.at[mine], send_sem=send_sem.at[j],
                                            recv_sem=recv_sem.at[j], device_id=device, device_id_type=MESH)
        copies.append(copy)
    return copies


def go(copies):
    for copy in copies:
        copy.start()


def finish(copies):
    for copy in copies:
        copy.wait()


def fold(values, parts):
    return sum(values[:, part] for part in parts)


def sum_slots(slots):
    total = slots[0]
    for j in range(1, slots.shape[0]):
        total = total + slots[j]
    return total


def gather_scratch(grid, block):
    n_chip, n_sw = grid[0] // 2, grid[1]
    dma = pltpu.SemaphoreType.DMA
    return [pltpu.VMEM((n,) + block, F32) for n in (2, n_chip, n_sw)] + [dma((max(n - 1, 1),)) for n in (2, 2, n_chip, n_chip, n_sw, n_sw)]


N_GATHER = 9


def gather_stages(grid, scratch):
    slots, sems = scratch[:3], scratch[3:]
    mine = [position()[1], position()[0], position()[2]]
    pair, row, col = peers_of(grid)
    copies = [exchange(slots[j], mine[j], devices, sems[2 * j], sems[2 * j + 1]) for j, devices in enumerate(([pair], row, col))]

    def stage(j):
        def run():
            if j > 0:
                finish(copies[j - 1])
            if j in (1, 2):
                slots[j][mine[j]] = sum_slots(slots[j - 1])
            if j < 3:
                go(copies[j])
        return run

    return [stage(j) for j in range(4)]


def grn_begin(dm, scratch, sums):
    core = position()[1]
    for j, ref in enumerate(sums):
        scratch[0][core, j] = fold(ref, dm.hs)


def grn_total(dm, grid, sums, scratch):
    grn_begin(dm, scratch, sums)
    for stage in gather_stages(grid, scratch):
        stage()
    return sum_slots(scratch[2])


def spread(dm, ref, values):
    ref[...] = jnp.zeros_like(ref)
    for part in dm.hs:
        ref[:, part] = values


def grn_cross(dm, norm, gamma, cross, dsq_o, ggam_o):
    mean = jnp.mean(norm, axis=-1, keepdims=True) + EPSILON
    d_scale = gamma * cross
    d_norm = d_scale / mean - jnp.sum(d_scale * norm, axis=-1, keepdims=True) / (mean * mean * dm.hid)
    spread(dm, dsq_o, d_norm / norm)
    ggam_o[...] = jnp.sum(cross * (norm / mean), axis=0, keepdims=True)


def grn_coef(dm, norm, gamma, coef_o):
    mean = jnp.mean(norm, axis=-1, keepdims=True) + EPSILON
    spread(dm, coef_o, gamma * (norm / mean) + 1.0)


def prep_kernel(dm, conv_w, conv_b, norm_g, norm_b, fc1_w, fc1_b, beta, fc2_t, fc2_b, mask_i, ones, place, perm, x, dout,
                taps_o, cvec_o, hvec_o, w1_o, w2t_o, gmat_o, mask_o, x_o, d_o):
    for ref in (taps_o, cvec_o, hvec_o, w1_o, w2t_o):
        ref[...] = jnp.zeros_like(ref)
    square = (dm.b, dm.b)
    diagonal = lax.broadcasted_iota(jnp.int32, square, 0) == lax.broadcasted_iota(jnp.int32, square, 1)
    for k in range(2):
        for cs, hs in zip(dm.cs, dm.hs):
            for j, ref in enumerate((conv_b, norm_g, norm_b, fc2_b)):
                cvec_o[k, j:j + 1, cs] = ref[k:k + 1, :]
            for j, ref in enumerate((fc1_b, beta)):
                hvec_o[k, j:j + 1, hs] = ref[k:k + 1, :]
            w1_o[k, cs, hs] = fc1_w[k]
            w2t_o[k, cs, hs] = fc2_t[k]
        column = jnp.sum(jnp.where(diagonal, mask_i[k:k + 1, :], 0.0), axis=1, keepdims=True)
        mask_o[k] = jnp.broadcast_to(column, (dm.b, dm.cp))
    for i in range(TAPS):
        for j in range(TAPS):
            both = conv_w[i, j].astype(F32)
            for k in range(2):
                for cs in dm.cs:
                    taps_o[k, pl.ds(i * 8 + j, 1), cs] = both[k:k + 1]
                    taps_o[2 + k, pl.ds((TAPS - 1 - i) * 8 + TAPS - 1 - j, 1), cs] = both[k:k + 1]
    for k in range(2):
        values = ones[...].astype(F32) * line(cvec_o, k, NORM_G)
        for j in range(3):
            part = values.astype(BF16)
            gmat_o[k, j] = part
            values = values - part.astype(F32)
    moves = move_rows(perm)
    for src, out in ((x, x_o), (dout, d_o)):
        for wg in range(dm.nw):
            joined = sum(dot(src[:, RADIUS * wg + q].reshape(-1, dm.c), place[q]) for q in range(RADIUS)).astype(BF16)
            moved = dot(moves, joined).astype(BF16)
            out[:, wg * dm.b:(wg + 1) * dm.b] = moved.reshape(dm.h, dm.b, dm.cp)


def first_kernel(dm, grid, x, taps, rel, cvec, hvec, ones, w1, gamma,
                 normed_o, inv_o, h_o, phi_o, xp_o, norm_o, coef_o, wide, toep, acc_s, ss, xp, keep_sem, send, recv, *grn):
    step = pl.program_id(0)

    @pl.when(step == 0)
    def _():
        clear_halo(dm, xp)
        for row in range(dm.h):
            xp[row + RADIUS, dm.inner] = x[row]
        greet(grid, True, True)
        sides, ends = halo_copies(dm, grid, xp, send, recv)
        halo_start(ends)
        halo_start(sides)
        build_toeplitz(dm, taps.at[0], rel, toep)
        ss[...] = jnp.zeros_like(ss)
        halo_wait(ends)
        build_wide(dm, xp, wide, ONE)

    @pl.when(step == dm.half)
    def _():
        halo_wait(halo_copies(dm, grid, xp, send, recv)[0])
        pltpu.make_async_copy(xp, xp_o, keep_sem).start()
        build_wide(dm, xp, wide, TWO)

    forward_tile(dm, ONE, step, wide, toep, acc_s, cvec, hvec, ones, w1, normed_o, inv_o, h_o)

    def body(rows, lanes):
        g = gelu_chunk(dm, h_o, phi_o, rows, lanes)
        ss[:, lanes] += jnp.sum(per_image(dm, g * g), axis=0)

    lane_loop(dm, body)

    @pl.when(step == pl.num_programs(0) - 1)
    def _():
        pltpu.make_async_copy(xp, xp_o, keep_sem).wait()
        norm = jnp.sqrt(grn_total(dm, grid, [ss], grn)[0])
        norm_o[...] = norm
        grn_coef(dm, norm, gamma[pl.ds(ONE, 1), :], coef_o)


def lead_tile(dm, step):
    return lax.rem(jnp.minimum(step, dm.tiles - 1) + dm.half, dm.tiles)


def halo_schedule(dm, grid, step, xp, wide, send, recv, between, after, ready=tuple):
    @pl.when(step == dm.half)
    def _():
        halo_start(halo_copies(dm, grid, xp, send, recv)[0])

    @pl.when(step == dm.tiles)
    def _():
        ends = halo_copies(dm, grid, xp, send, recv)[1]
        halo_start(ends)
        between()
        halo_wait(ends)
        build_wide(dm, xp, wide, ONE)
        ready()

    @pl.when(step == dm.tiles + dm.half)
    def _():
        halo_wait(halo_copies(dm, grid, xp, send, recv)[0])
        after()
        build_wide(dm, xp, wide, TWO)


def second_kernel(dm, grid, h1, phi1, xp1, coef1, taps, rel, cvec, hvec, ones, w1, w2t, gamma, mask, dout,
                  normed_o, inv_o, h_o, phi_o, dr_o, xp_o, sdr_o, coef_o, dsq_o, ggam_o,
                  wide, toep, acc_s, resp, raw, ss, cross, tile_s, xp, keep_sem, send, recv, *grn):
    step = pl.program_id(0)
    keep = pltpu.make_async_copy(xp, xp_o, keep_sem)

    @pl.when(step == 0)
    def _():
        clear_halo(dm, xp)
        greet(grid, True, True)
        for ref in (ss, cross, sdr_o):
            ref[...] = jnp.zeros_like(ref)

    halo_schedule(dm, grid, step, xp, wide, send, recv, lambda: build_toeplitz(dm, taps.at[1], rel, toep), keep.start)

    @pl.when(step < dm.tiles)
    def _():
        tile = lead_tile(dm, step)

        def body(rows, lanes):
            g = h1[rows, lanes].astype(F32) * phi1[rows, lanes]
            r = per_image(dm, g) * image_lines(coef1, lanes) + line(hvec, ONE, BETA, lanes)
            resp[rows, lanes] = r.reshape(dm.chunk, 128).astype(BF16)

        lane_loop(dm, body)
        load_tile(dm, xp1, tile_s, tile, dm.b, RADIUS)
        o = (dot_bt(resp[:, :dm.hp], w2t[ONE, :, :dm.hp]) + line(cvec, ONE, FC2_B)).reshape(-1, dm.b, dm.cp)
        y = (tile_s[...].astype(F32) + (o * mask[ONE][None]).reshape(-1, dm.cp)).astype(BF16)
        store_tile(dm, xp, y, tile, dm.b, RADIUS)

    @pl.when(step >= dm.tiles)
    def _():
        tile = step - dm.tiles
        forward_tile(dm, TWO, tile, wide, toep, acc_s, cvec, hvec, ones, w1, normed_o, inv_o, h_o)
        load_tile(dm, dout, tile_s, tile, 0, 0)
        raw[...] = dot(tile_s[...], w2t[TWO, :, :dm.hp])

        def body(rows, lanes):
            g = gelu_chunk(dm, h_o, phi_o, rows, lanes)
            ss[:, lanes] += jnp.sum(per_image(dm, g * g), axis=0)
            cross_chunk(dm, TWO, raw, mask, g, dr_o, cross, sdr_o, rows, lanes)

        lane_loop(dm, body)

    @pl.when(step == pl.num_programs(0) - 1)
    def _():
        keep.wait()
        total = grn_total(dm, grid, [ss, cross], grn)
        norm = jnp.sqrt(total[0])
        grn_coef(dm, norm, gamma[pl.ds(TWO, 1), :], coef_o)
        grn_cross(dm, norm, gamma[pl.ds(TWO, 1), :], total[1], dsq_o, ggam_o)


def backward_tile(dm, k, h_i, phi_i, dr_i, coef, dsq, dout, normed_i, inv_i, cvec, hvec, ones, gmat, w1, w2t, mask,
                  resp, dh, gfc1, gfc2, sdh, sums, x_rows):
    def body(rows, lanes):
        hv = h_i[rows, lanes].astype(F32)
        phi = phi_i[rows, lanes]
        g = per_image(dm, hv * phi)
        a = image_lines(coef, lanes)
        resp[rows, lanes] = (g * a + line(hvec, k, BETA, lanes)).reshape(dm.chunk, 128).astype(BF16)
        slope = phi + hv * (np.float32(0.3989422804014327) * jnp.exp(-0.5 * hv * hv))
        dg = per_image(dm, dr_i[rows, lanes].astype(F32)) * a + g * image_lines(dsq, lanes)
        dhv = (dg.reshape(dm.chunk, 128) * slope).astype(BF16)
        dh[rows, lanes] = dhv
        sdh[:, lanes] += jnp.sum(per_image(dm, dhv.astype(F32)), axis=0)

    lane_loop(dm, body)
    dsel32 = jnp.where((mask[k] != 0.0)[None], dout[...].astype(F32).reshape(-1, dm.b, dm.cp), 0.0)
    sums[FC2_B] += jnp.sum(dsel32, axis=0)
    gfc2[...] += dot_t(dsel32.reshape(-1, dm.cp).astype(BF16), resp[:, :dm.hp])
    y = None
    if x_rows is not None:
        o = (dot_bt(resp[:, :dm.hp], w2t[k, :, :dm.hp]) + line(cvec, k, FC2_B)).reshape(-1, dm.b, dm.cp)
        y = (x_rows[...].astype(F32) + (o * mask[k][None]).reshape(-1, dm.cp)).astype(BF16)
    normed = normed_i[...]
    norm_g = line(cvec, k, NORM_G)
    n = (normed * norm_g + line(cvec, k, NORM_B)).astype(BF16)
    gfc1[...] += dot_t(n, dh[:, :dm.hp])
    dn16 = dot_bt(dh[:, :dm.hp], w1[k, :, :dm.hp]).astype(BF16)
    dn = dn16.astype(F32)
    scale = np.float32(1.0 / dm.c)
    mean1 = (dot_bt(dn16, gmat[k, 0]) + dot_bt(dn16, gmat[k, 1]) + dot_bt(dn16, gmat[k, 2])) * scale
    dnormed = dn * norm_g
    mean2 = dot_split(dnormed * normed, ones[...]) * scale
    dconv = (inv_i[...] * (dnormed - mean1 - normed * mean2)).astype(BF16)

    for row, values in ((CONV_B, dconv.astype(F32)), (NORM_G, dn * normed), (NORM_B, dn)):
        sums[row] += jnp.sum(values.reshape(-1, dm.b, dm.cp), axis=0)
    return dconv, y


def wgrad(dm, wide, dcol, rel, out, stages):
    keep = rel[...] > -50

    def body(i, carry):
        res = None
        for pair in range(2):
            rows = pl.ds(pl.multiple_of(pair * dm.tall + i * dm.rw, 16), dm.block)
            part = dot(dcol[:, pair * dm.block:(pair + 1) * dm.block], wide[rows, :])
            res = part if res is None else res + part
        for g in range(RADIUS):
            part = jnp.where(keep, res[:, dm.lanes(g)], 0.0)
            for q in range(RADIUS):
                out[q, pl.ds(i, 1), dm.lanes(g)] = jnp.sum(part[dm.cs[q]], axis=0, keepdims=True)
        for tap, stage in stages.items():
            pl.when(i == tap)(stage)
        return carry

    loop(TAPS, body)


def vector_rows(dm):
    return 2 * dm.c


def conv_rows(dm):
    return round_up(2 * dm.c + 6, 8)


def pack_conv(dm, out, base, corr):
    for j in range(TAPS):
        total = None
        for q in range(RADIUS):
            lane = ((q + j) // RADIUS) * dm.cp + ((q + j) % RADIUS) * dm.c
            part = corr[q, :, lane:lane + dm.c]
            total = part if total is None else total + part
        out[base + 8 * j:base + 8 * j + 8, :dm.c] = total


def pack_grads(dm, pack, gfc1, gfc2, sdh, sdr, sums):
    for base, ref in ((0, gfc1), (dm.c, gfc2)):
        pack[base:base + dm.c, :dm.hid] = sum(ref[cs, hs] for cs, hs in zip(dm.cs, dm.hs))
    base = vector_rows(dm)
    rows = [fold(jnp.sum(ref[...], axis=0, keepdims=True), dm.hs) for ref in (sdh, sdr)]
    rows += [fold(jnp.sum(sums[row], axis=0, keepdims=True), dm.cs) for row in range(4)]
    for j, row in enumerate(rows):
        pack[base + j:base + j + 1, :row.shape[1]] = row


def pack_shape(dm, grid, conv):
    rows = conv_rows(dm) + (8 * TAPS if conv else 0)
    return (round_up(rows, 8 * grid[0]), round_up(dm.hid, 128))


def conv_shape(dm):
    return (8 * TAPS, 128)


def sum_scratch(grid, shape):
    rows, lanes = shape
    n_chip, n_sw = grid[0] // 2, grid[1]
    dma = pltpu.SemaphoreType.DMA
    return ([pltpu.VMEM((rows // 2, lanes), F32)]
            + [pltpu.VMEM((n, rows // (2 * n_chip), lanes), F32) for n in (n_chip, n_chip, n_chip, n_sw)]
            + [dma((n,)) for n in (1, 1, n_chip - 1, n_chip - 1, n_sw - 1, n_sw - 1, n_chip - 1, n_chip - 1, 1, 1)])


N_SUM = 15


def sum_stages(grid, x, out, scratch):
    got1, half, got2, part, slots3, send1, recv1, send2, recv2, send3, recv3, send4, recv4, send5, recv5 = scratch
    chip, core, sw = position()
    n_chip = grid[0] // 2
    pair, row, col = peers_of(grid)
    rows = got1.shape[0]
    chunk = half.shape[1]

    def whole(ref, which):
        return ref.at[pl.ds(pl.multiple_of(which * rows, 8), rows)]

    def copies1():
        return [pltpu.make_async_remote_copy(src_ref=whole(x, 1 - core), dst_ref=got1, send_sem=send1.at[0], recv_sem=recv1.at[0],
                                             device_id=pair, device_id_type=MESH)]

    def copies2():
        made = []
        for j, device in enumerate(row):
            made.append(pltpu.make_async_remote_copy(
                src_ref=half.at[lax.rem(chip + j + 1, n_chip)], dst_ref=got2.at[chip], send_sem=send2.at[j],
                recv_sem=recv2.at[j], device_id=device, device_id_type=MESH))
        return made

    def copies5():
        return [pltpu.make_async_remote_copy(src_ref=whole(out, core), dst_ref=whole(out, core), send_sem=send5.at[0],
                                             recv_sem=recv5.at[0], device_id=pair, device_id_type=MESH)]

    def stage0():
        go(copies1())

    def stage1():
        finish(copies1())
        for j in range(n_chip):
            start = pl.multiple_of(core * rows + j * chunk, 8)
            half[j] = x[pl.ds(start, chunk)] + got1[j * chunk:(j + 1) * chunk]
        go(copies2())

    def stage2():
        got2[chip] = half[chip]
        finish(copies2())
        slots3[sw] = sum_slots(got2)
        go(exchange(slots3, sw, col, send3, recv3))

    def stage3():
        finish(exchange(slots3, sw, col, send3, recv3))
        part[chip] = sum_slots(slots3)
        go(exchange(part, chip, row, send4, recv4))

    def stage4():
        finish(exchange(part, chip, row, send4, recv4))
        for j in range(n_chip):
            out[pl.ds(pl.multiple_of(core * rows + j * chunk, 8), chunk)] = part[j]
        go(copies5())

    def stage5():
        finish(copies5())

    return [stage0, stage1, stage2, stage3, stage4, stage5]


def backward_phase(dm, step, k, dp, dcol, args, x_rows):
    tile = lead_tile(dm, step)
    dconv, y = backward_tile(dm, k, *args, x_rows)
    store_tile(dm, dp, dconv, tile, dm.b, RADIUS)
    dcol[:, pl.ds(pl.multiple_of(tile * dm.m, 128), dm.m)] = dconv.T
    return tile, y


def third_kernel(dm, grid, h2, phi2, dr2, coef2, dsq2, dout, normed, inv, xp2, h1, phi1, norm1, taps, rel, cvec, hvec, ones, gmat,
                 w1, w2t, gamma, mask, sdr2,
                 y_o, d1_o, dr1_o, pack, sdr_o, dsq_o, ggam_o,
                 wide, toep, acc_s, dp, dcol, corr, resp, dh, tile_s, gfc1, gfc2, sdh, sums, raw, tile_x, cross, send, recv, *grn):
    step = pl.program_id(0)

    @pl.when(step == 0)
    def _():
        clear_halo(dm, dp)
        greet(grid, True, True)
        for ref in (cross, sdr_o, gfc1, gfc2, sdh, sums, corr, pack):
            ref[...] = jnp.zeros_like(ref)

    halo_schedule(dm, grid, step, dp, wide, send, recv, lambda: build_toeplitz(dm, taps.at[3], rel, toep), tuple)

    @pl.when(step < dm.tiles)
    def _():
        load_tile(dm, dout, tile_s, lead_tile(dm, step), 0, 0)
        load_tile(dm, xp2, tile_x, lead_tile(dm, step), dm.b, RADIUS)
        tile, y = backward_phase(dm, step, TWO, dp, dcol, (h2, phi2, dr2, coef2, dsq2, tile_s, normed, inv, cvec, hvec, ones, gmat,
                                                           w1, w2t, mask, resp, dh, gfc1, gfc2, sdh, sums), tile_x)
        store_tile(dm, y_o, y, tile, 0, 0)

    @pl.when(step >= dm.tiles)
    def _():
        tile = step - dm.tiles
        load_tile(dm, dout, tile_s, tile, 0, 0)
        din = (tile_s[...].astype(F32) + conv_tile(dm, wide, toep, tile, acc_s)).astype(BF16)
        d1_o[...] = din
        raw[...] = dot(din, w2t[ONE, :, :dm.hp])

        def body(rows, lanes):
            g = h1[rows, lanes].astype(F32) * phi1[rows, lanes]
            cross_chunk(dm, ONE, raw, mask, g, dr1_o, cross, sdr_o, rows, lanes)

        lane_loop(dm, body)

    @pl.when(step == pl.num_programs(0) - 1)
    def _():
        begin, row, col, end = gather_stages(grid, grn)
        grn_begin(dm, grn, [cross])
        begin()
        build_wide(dm, xp2, wide, ONE)
        build_wide(dm, xp2, wide, TWO)
        pack_grads(dm, pack, gfc1, gfc2, sdh, sdr2, sums)
        wgrad(dm, wide, dcol, rel, corr, {ONE: row, RADIUS: col})
        pack_conv(dm, pack, conv_rows(dm), corr)
        end()
        grn_cross(dm, norm1[...], gamma[pl.ds(ONE, 1), :], sum_slots(grn[2])[0], dsq_o, ggam_o)


def fourth_kernel(dm, grid, h1, phi1, dr1, coef1, dsq1, d1, normed, inv, xp1, taps, rel, cvec, hvec, ones, gmat,
                  w1, w2t, mask, sdr1, pack2_i,
                  d0_o, out1_o, out2_o, conv_o,
                  wide, toep, acc_s, dp, dcol, corr, resp, dh, tile_s, gfc1, gfc2, sdh, sums, pack1, out1, pack2, out2, send, recv, *sem):
    step = pl.program_id(0)
    stages1 = sum_stages(grid, pack1, out1, sem[:N_SUM])
    stages2 = sum_stages(grid, pack2, out2, sem[N_SUM:2 * N_SUM])
    conv_sem = sem[2 * N_SUM:]
    conv_stages = gather_stages(grid, conv_sem)

    @pl.when(step == 0)
    def _():
        clear_halo(dm, dp)
        greet(grid, True, True)
        for ref in (gfc1, gfc2, sdh, sums, corr, pack1):
            ref[...] = jnp.zeros_like(ref)
        pack2[...] = pack2_i[...]

    begin1, *middle1, end1 = stages1
    conv_begin, conv_row, conv_col, conv_end = conv_stages
    a, b, c, d, e, f = stages2
    plan = [[a], [b], [], [c], [d], [e], [], [f, conv_col], [], [middle1.pop()]]
    for at, jobs in enumerate(plan):
        @pl.when(step == at)
        def _():
            for job in jobs:
                job()

    def between():
        pack_grads(dm, pack1, gfc1, gfc2, sdh, sdr1, sums)
        begin1()
        build_toeplitz(dm, taps.at[2], rel, toep)
        build_wide(dm, xp1, wide, ONE)
        build_wide(dm, xp1, wide, TWO)
        half, chip, column = middle1
        half()
        wgrad(dm, wide, dcol, rel, corr, {RADIUS: chip})
        core = position()[1]
        conv_sem[0][core] = jnp.zeros(conv_shape(dm), F32)
        pack_conv(dm, conv_sem[0].at[core], 0, corr)
        conv_begin()
        column()

    halo_schedule(dm, grid, step, dp, wide, send, recv, between, tuple, conv_row)

    @pl.when(step < dm.tiles)
    def _():
        backward_phase(dm, step, ONE, dp, dcol, (h1, phi1, dr1, coef1, dsq1, d1, normed, inv, cvec, hvec, ones, gmat,
                                                 w1, w2t, mask, resp, dh, gfc1, gfc2, sdh, sums), None)

    @pl.when(step >= dm.tiles)
    def _():
        tile = step - dm.tiles
        din = (d1[...].astype(F32) + conv_tile(dm, wide, toep, tile, acc_s)).astype(BF16)
        store_tile(dm, d0_o, din, tile, 0, 0)

    @pl.when(step == pl.num_programs(0) - 1)
    def _():
        end1()
        out1_o[...] = out1[...]
        out2_o[...] = out2[...]
        conv_end()
        conv_o[...] = sum_slots(conv_sem[2])


def final_kernel(dm, out1, out2, conv1, ggam1, ggam2, y, d, place, perm, yo, do, gcw, gcb, gng, gnb, gf1w, gf1b, ggam, gbeta, gf2w, gf2b):
    c, hid = dm.c, dm.hid
    ggam[...] = jnp.concatenate([ggam1[...], ggam2[...]], axis=0)
    for k, ref in enumerate((out1, out2)):
        gf1w[k] = ref[:c, :hid]
        gf2w[k] = ref[c:2 * c, :hid] * np.float32(KEEP)
        base = vector_rows(dm)
        for row, out in enumerate((gf1b, gbeta, gcb, gng, gnb, gf2b)):
            value = ref[base + row:base + row + 1, :out.shape[1]]
            out[k:k + 1, :] = value * np.float32(KEEP) if out is gf2b else value
    for k, (ref, base) in enumerate(((conv1, 0), (out2, conv_rows(dm)))):
        for j in range(TAPS):
            for i in range(TAPS):
                row = base + 8 * j + i
                gcw[i, j, k:k + 1, :] = ref[row:row + 1, :c]
    moves = move_rows(perm)
    for src, out in ((y, yo), (d, do)):
        for wg in range(dm.nw):
            rows = src[:, wg * dm.b:(wg + 1) * dm.b].reshape(-1, dm.cp)
            moved = dot(moves, rows).astype(BF16)
            for q in range(RADIUS):
                out[:, RADIUS * wg + q] = dot_bt(moved, place[q]).astype(BF16).reshape(dm.b, dm.h, dm.c)


def constants(dm):
    index = np.arange(dm.cp)
    col, chan = index // dm.c, index % dm.c
    live = (index[:, None] < RADIUS * dm.c) & (index[None, :] < RADIUS * dm.c)
    rel = np.where((chan[:, None] == chan[None, :]) & live, col[:, None] - col[None, :], -100).astype(np.int32)
    ones = ((col[:, None] == col[None, :]) & live).astype(np.float32)
    place = np.stack([np.eye(dm.c, dm.cp, q * dm.c) for q in range(RADIUS)])
    count = dm.h * dm.b
    order = np.arange(count, dtype=np.int32)
    moves = [order.reshape(shape).T.reshape(1, count) for shape in ((dm.h, dm.b), (dm.b, dm.h))]
    return [jnp.asarray(a) for a in [rel] + moves] + [jnp.asarray(a, BF16) for a in (ones, place)]


def move_rows(ref):
    count = ref.shape[1]
    rows = lax.broadcasted_iota(jnp.int32, (count, count), 0)
    return jnp.where(rows == ref[...], 1.0, 0.0).astype(BF16)


def call(dm, kernel, steps, ins, outs, scratch, name, cid):
    def spec(shape, mode):
        if mode is WHOLE:
            return FULL
        if mode == 'any':
            return pl.BlockSpec(memory_space=pl.ANY)
        maps = {'lead': lambda s: (lead_tile(dm, s), 0),
                'tail': lambda s: (jnp.maximum(s - dm.tiles, 0), 0),
                'both': lambda s: (jnp.where(s < dm.tiles, lead_tile(dm, s), s - dm.tiles), 0),
                'only': lambda s: (s, 0)}
        return pl.BlockSpec((dm.m, shape[1]), maps[mode])

    return pl.pallas_call(
        kernel, grid=(steps,), in_specs=[spec(a.shape, mode) for a, mode in ins],
        out_specs=[spec(shape, mode) for shape, _, mode in outs],
        out_shape=[jax.ShapeDtypeStruct(shape, dtype) for shape, dtype, _ in outs],
        scratch_shapes=scratch, name=name,
        compiler_params=pltpu.CompilerParams(dimension_semantics=('arbitrary',), vmem_limit_bytes=VMEM_LIMIT,
                                             collective_id=cid, has_side_effects=True))(*[a for a, _ in ins])


def solution(mesh):
    grid = (mesh.shape['sh'], mesh.shape['sw'])
    act_spec = P('dp', 'sh', 'sw', WHOLE)
    replicated = P()

    def local_step(act_in, drop_mask, grad_out, conv_w, conv_b, norm_g, norm_b, fc1_w, fc1_b, gamma, grn_beta, fc2_w, fc2_b):
        dm = Dims(act_in.shape, fc1_w.shape[-1])
        rel, perm, perm_back, ones, place = constants(dm)
        sds = jax.ShapeDtypeStruct
        c_shape, h_shape, p_shape, s_shape, n_shape = (dm.rows, dm.cp), (dm.rows, dm.hp), (dm.rows, dm.pitch), (dm.b, dm.hp), (dm.b, dm.hid)
        x_shape = (dm.h, dm.nw * dm.b, dm.cp)
        act_t = (dm.b, dm.w, dm.h, dm.c)
        swap = (0, 2, 1, 3)
        big = pltpu.CompilerParams(vmem_limit_bytes=VMEM_LIMIT)
        taps, cvec, hvec, w1, w2t, gmat, mask, x1, d2 = pl.pallas_call(
            functools.partial(prep_kernel, dm),
            out_shape=[sds((4, TAPS * 8, dm.cp), F32), sds((2, 4, dm.cp), F32), sds((2, 2, dm.hp), F32), sds((2, dm.cp, dm.pitch), BF16),
                       sds((2, dm.cp, dm.pitch), BF16), sds((2, 3, dm.cp, dm.cp), BF16), sds((2, dm.b, dm.cp), F32),
                       sds(x_shape, BF16), sds(x_shape, BF16)],
            in_specs=[FULL] * 15, out_specs=[FULL] * 9, compiler_params=big, name='prep')(
                conv_w.transpose(1, 2, 0, 3), conv_b, norm_g, norm_b, fc1_w, fc1_b, grn_beta, fc2_w.transpose(0, 2, 1), fc2_b,
                drop_mask.T, ones, place, perm, act_in.transpose(swap), grad_out.transpose(swap))

        dma = pltpu.SemaphoreType.DMA
        V = pltpu.VMEM
        wide_s = V((2 * dm.tall, 3 * dm.cp), BF16)
        toep_s = V((TAPS * 3 * dm.cp, dm.cp), BF16)
        raw_s, hid_s, tile_s = V((dm.m, dm.hp), F32), V((dm.m, dm.pitch), BF16), V((dm.m, dm.cp), BF16)
        conv_s = V((dm.block, dm.cp), F32)
        img_s, acc_s = V(s_shape, F32), V((dm.cp, dm.hp), F32)
        xp_shape = (dm.h + 2 * RADIUS, (dm.nw + 2) * dm.b, dm.cp)
        xp_s = V(xp_shape, BF16)
        halo_s = [dma((8,)), dma((8,))]
        g_shape = (1, dm.hid)
        p1_shape, p2_shape = (pack_shape(dm, grid, conv) for conv in (False, True))

        def wholes(*arrays):
            return [(a, WHOLE) for a in arrays]

        def grn_s(count):
            return gather_scratch(grid, (count, dm.b, dm.hid))

        normed1, inv1, h1, phi1, xp1, norm1, coef1 = call(
            dm, functools.partial(first_kernel, dm, grid), dm.tiles, wholes(x1, taps, rel, cvec, hvec, ones, w1, gamma),
            [(c_shape, F32, 'only'), (c_shape, F32, 'only'), (p_shape, BF16, 'only'), (h_shape, F32, 'only'), (xp_shape, BF16, 'any'),
             (n_shape, F32, WHOLE), (s_shape, F32, WHOLE)],
            [wide_s, toep_s, conv_s, img_s, xp_s, dma] + halo_s + grn_s(1), 'first', 0)

        normed2, inv2, h2, phi2, dr2, xp2, sdr2, coef2, dsq2, ggam2 = call(
            dm, functools.partial(second_kernel, dm, grid), 2 * dm.tiles,
            [(h1, 'lead'), (phi1, 'lead')] + wholes(xp1, coef1, taps, rel, cvec, hvec, ones, w1, w2t, gamma, mask, d2),
            [(c_shape, F32, 'tail'), (c_shape, F32, 'tail'), (p_shape, BF16, 'tail'), (h_shape, F32, 'tail'), (p_shape, BF16, 'tail'),
             (xp_shape, BF16, 'any')] + [(s_shape, F32, WHOLE)] * 3 + [(g_shape, F32, WHOLE)],
            [wide_s, toep_s, conv_s, hid_s, raw_s, img_s, img_s, tile_s, xp_s, dma] + halo_s + grn_s(2), 'second', 1)

        bwd_s = [wide_s, toep_s, conv_s, xp_s, V((dm.cp, dm.rows), BF16), V((3, 8, 3 * dm.cp), F32), hid_s, hid_s, tile_s,
                 acc_s, acc_s, img_s, V((4, dm.b, dm.cp), F32)]
        y2, d1, dr1, pack2, sdr1, dsq1, ggam1 = call(
            dm, functools.partial(third_kernel, dm, grid), 2 * dm.tiles,
            [(h2, 'lead'), (phi2, 'lead'), (dr2, 'lead')] + wholes(coef2, dsq2, d2) + [(normed2, 'lead'), (inv2, 'lead')] + wholes(xp2)
            + [(h1, 'tail'), (phi1, 'tail')] + wholes(norm1, taps, rel, cvec, hvec, ones, gmat, w1, w2t, gamma, mask, sdr2),
            [(x_shape, BF16, WHOLE), (c_shape, BF16, 'tail'), (p_shape, BF16, 'tail'), (p2_shape, F32, WHOLE), (s_shape, F32, WHOLE),
             (s_shape, F32, WHOLE), (g_shape, F32, WHOLE)],
            bwd_s + [raw_s, tile_s, img_s] + halo_s + grn_s(1), 'third', 2)

        d0, out1, out2, conv1 = call(
            dm, functools.partial(fourth_kernel, dm, grid), 2 * dm.tiles,
            [(h1, 'lead'), (phi1, 'lead'), (dr1, 'lead')] + wholes(coef1, dsq1) + [(d1, 'both'), (normed1, 'lead'), (inv1, 'lead')]
            + wholes(xp1, taps, rel, cvec, hvec, ones, gmat, w1, w2t, mask, sdr1, pack2),
            [(x_shape, BF16, WHOLE), (p1_shape, F32, WHOLE), (p2_shape, F32, WHOLE), (conv_shape(dm), F32, WHOLE)],
            bwd_s + [V(p1_shape, F32)] * 2 + [V(p2_shape, F32)] * 2 + halo_s + sum_scratch(grid, p1_shape) + sum_scratch(grid, p2_shape)
            + gather_scratch(grid, conv_shape(dm)), 'fourth', 3)

        conv_t, fc2_t = (TAPS, TAPS, 2, dm.c), (2, dm.c, dm.hid)
        y_t, d_t, gcw, gcb, gng, gnb, gf1w, gf1b, ggam, gbeta, gf2w, gf2b = pl.pallas_call(
            functools.partial(final_kernel, dm),
            out_shape=[sds(act_t, BF16)] * 2 + [sds(shape, F32) for shape in (
                conv_t, conv_b.shape, norm_g.shape, norm_b.shape, fc1_w.shape, fc1_b.shape, gamma.shape, grn_beta.shape, fc2_t, fc2_b.shape)],
            in_specs=[FULL] * 9, out_specs=[FULL] * 12, compiler_params=big, name='final')(
                out1, out2, conv1, ggam1, ggam2, y2, d0, place, perm_back)
        return (y_t.transpose(swap), d_t.transpose(swap), gcw.transpose(2, 0, 1, 3), gcb, gng, gnb, gf1w, gf1b, ggam, gbeta,
                gf2w.transpose(0, 2, 1), gf2b)

    return jax.shard_map(local_step, mesh=mesh,
                         in_specs=(act_spec, P('dp', WHOLE), act_spec) + (replicated,) * 10,
                         out_specs=(act_spec, act_spec) + (P('dp'),) * 10,
                         check_vma=False)
```
